32 devices in a mesh: row: 4 (over y, core), col: 8 (over z, x).
Axes of the slice: x: 2, y: 2, z: 4, core: 2. Of those that a mesh axis runs over, the one named last changes fastest.
Arguments:
- excitons: float32 [1024, 1024], P('row', 'col'), may hold values from -500 to 500
- valence_energy: float32 [1024], P('row'), may hold values from -3 to -1
- conduction_energy: float32 [1024], P('col'), may hold values from 1 to 3
- psi_valence: float32 [4096, 1024], P('row', 'col'), may hold values from -0.1875 to 0.1875
- psi_conduction: float32 [4096, 1024], P('col', 'row'), may hold values from -0.1875 to 0.1875
- screened: float32 [4096, 4096], P('row', 'col'), may hold values from -0.9 to 0.975, as said below
Outputs:
- next_vector: float32 [1024, 1024], P('row', 'col')
- coefficients: float32 [4], replicated
The draws below stay inside these ranges and needn't reach their ends.
Inputs may be any that keep to these rules, and one draw needn't show every extreme that they name: symmetric: screened[p, p'] = screened[p', p].
All inputs are finite; a program needn't handle non-finite values.
Results may differ from the reference program's by a relative error of at most 0.0003.
Values sent between devices are 32-bit elements; how exact they have to be, the bound alone decides.
A program may use at most 64 MiB of HBM per device.

```python
import math
import jax
import jax.numpy as jnp
from jax import lax

NV = 1024
NC = 1024
NP = 4096
STEPS = 2


def draw_excitons(key, part):
    base_key = jax.random.fold_in(key, 11)
    key_entries, key_rows, key_cols = jax.random.split(base_key, 3)
    row_scale = 3.0 ** (jnp.arange(NV, dtype=jnp.float32) / NV) * jnp.exp(jax.random.uniform(key_rows, (NV,), jnp.float32, 0.0, math.log(3.2)))
    col_scale = 3.0 ** (jnp.arange(NC, dtype=jnp.float32) / NC) * jnp.exp(jax.random.uniform(key_cols, (NC,), jnp.float32, 0.0, math.log(3.2)))
    entries = jnp.clip(jax.random.normal(key_entries, (NV, NC), jnp.float32), -5.0, 5.0)
    return (entries * row_scale[:, None] * col_scale[None, :]).astype(jnp.float32)


def draw_screened(key, part):
    base_key = jax.random.fold_in(key, 23)
    noise_scale = 0.6 * (NV * NC) ** 0.5 / NP
    smooth_height = 1.2 * NV * NC / (NP * NP)
    places = jnp.arange(NP, dtype=jnp.float32)
    distance = jnp.abs(places[:, None] - places[None, :])
    noise = jnp.clip(jax.random.normal(base_key, (NP, NP), jnp.float32), -4.0, 4.0)
    reach = NP / 8.0
    symmetric = (noise + noise.T) * (1.0 / math.sqrt(2.0))
    smooth = smooth_height * jnp.exp(-distance / reach)
    return (noise_scale * symmetric + smooth).astype(jnp.float32)


def levels(own_key, shape, pieces, smallest, largest):
    level = 1.0
    for axis_at, parts in pieces:
        steps = jax.random.uniform(jax.random.fold_in(jax.random.fold_in(own_key, 6), axis_at), (parts,), jnp.float32, smallest / len(pieces), largest / len(pieces))
        level = level * jnp.repeat(jnp.exp(steps), shape[axis_at] // parts).reshape((-1,) + (1,) * (len(shape) - 1 - axis_at))
    return level


def normal_values(stream_key, shape, deviation, limit, shards=(), kind=jnp.bfloat16):
    array = jax.random.normal(stream_key, shape, jnp.float32) * deviation
    if len(shards) > 0:
        array = levels(stream_key, shape, shards, -0.22, 0.18) * array
    return jnp.clip(array, min=-limit, max=limit).astype(kind)


def setup_inputs(seed: int = 0) -> dict:
    seeds = jax.random.split(jax.random.key(seed), 7)
    return {
        "excitons": draw_excitons(jax.random.fold_in(seeds[6], 71), 0),
        "valence_energy": jnp.clip(-3.0 + 2.0 * jax.random.uniform(seeds[1], (NV,), jnp.float32) ** levels(seeds[1], (NV,), ((0, 4),), -0.2, 0.2), -3.0, -1.0),
        "conduction_energy": jnp.clip(1.0 + 2.0 * jax.random.uniform(seeds[2], (NC,), jnp.float32) ** levels(seeds[2], (NC,), ((0, 8),), -0.2, 0.2), 1.0, 3.0),
        "psi_valence": normal_values(seeds[3], (NP, NV), NV ** -0.5, 0.1875, ((0, 4), (1, 8)), jnp.float32),
        "psi_conduction": normal_values(seeds[4], (NP, NC), NC ** -0.5, 0.1875, ((0, 8), (1, 4)), jnp.float32),
        "screened": draw_screened(jax.random.fold_in(seeds[6], 71), 0),
    }


EPS = 1e-06

def inner(left, right):
    return jnp.sum(left * right) / (NV * NC)

def apply_operator(vector, valence_energy, conduction_energy, psi_valence, psi_conduction, screened):
    high = lax.Precision.HIGHEST
    image = jnp.dot(vector, psi_conduction.T, precision=high)
    points = jnp.dot(psi_valence, image, precision=high)
    weighted = points * screened
    back_valence = jnp.dot(psi_valence.T, weighted, precision=high)
    kernel = jnp.dot(back_valence, psi_conduction, precision=high)
    energy_gap = conduction_energy[None, :] - valence_energy[:, None]
    return energy_gap * vector - kernel

def reference(excitons, valence_energy, conduction_energy, psi_valence, psi_conduction, screened):
    vector = excitons / jnp.sqrt(inner(excitons, excitons) + EPS)
    previous = jnp.zeros_like(vector)
    beta_prev = jnp.zeros((), jnp.float32)
    values = []
    for step in range(STEPS):
        image = apply_operator(vector, valence_energy, conduction_energy, psi_valence, psi_conduction, screened)
        alpha = inner(vector, image)
        residual = image - alpha * vector - beta_prev * previous
        beta = jnp.sqrt(inner(residual, residual) + EPS)
        previous = vector
        vector = residual / beta
        beta_prev = beta
        values.append(alpha)
        values.append(beta)
    return (vector, jnp.stack(values))
```

```python
import jax
import jax.numpy as jnp
from jax import lax
from jax.experimental import pallas as pl
from jax.experimental.pallas import tpu as pltpu
from jax.sharding import PartitionSpec as P

NV = 1024
NC = 1024
STEPS = 2


EPS = 1e-06


def shards(excitons, valence_energy, conduction_energy, psi_valence, psi_conduction, screened):
    high = lax.Precision.HIGHEST
    count = NV * NC
    energy_gap = conduction_energy[None, :] - valence_energy[:, None]
    total = lax.psum(jnp.sum(excitons * excitons), ("row", "col"))
    vector = excitons / jnp.sqrt(total / count + EPS)
    previous = jnp.zeros_like(vector)
    beta_prev = jnp.zeros((), jnp.float32)
    values = []
    for step in range(STEPS):
        panel_valence = lax.all_gather(psi_valence, "col", axis=1, tiled=True)
        panel_conduction = lax.all_gather(psi_conduction, "row", axis=1, tiled=True)
        full_rows = lax.all_gather(vector, "col", axis=1, tiled=True)
        image_block = jnp.dot(full_rows, panel_conduction.T, precision=high)
        image_columns = lax.all_gather(image_block, "row", axis=0, tiled=True)
        points = jnp.dot(panel_valence, image_columns, precision=high)
        weighted = points * screened
        back_valence = lax.psum_scatter(
            jnp.dot(panel_valence.T, weighted, precision=high),
            "row",
            scatter_dimension=0,
            tiled=True,
        )
        back_flipped = back_valence.T
        kernel_flipped = lax.psum_scatter(
            jnp.dot(panel_conduction.T, back_flipped, precision=high),
            "col",
            scatter_dimension=0,
            tiled=True,
        )
        image = energy_gap * vector - kernel_flipped.T
        cross, square, older = lax.psum(
            (jnp.sum(vector * image), jnp.sum(image * image), jnp.sum(previous * image)),
            ("row", "col"),
        )
        alpha = cross / count
        residual = image - alpha * vector - beta_prev * previous
        squared = (
            square / count - alpha * alpha - 2.0 * beta_prev * older / count + beta_prev * beta_prev
        )
        beta = jnp.sqrt(squared + EPS)
        previous = vector
        vector = residual / beta
        beta_prev = beta
        values.append(alpha)
        values.append(beta)
    return (vector, jnp.stack(values))


MESH = pl.DeviceIdType.MESH
NN = (((1,), (0,)), ((), ()))
NT = (((1,), (1,)), ((), ()))
CHUNKS = 4
PIECES = 4
OPENING = (
    "t", "f0", "f1", "o2", "w3", "f2", "w2", "w1", "q", "o3", "a30", "c", "o1", "i",
    "x30", "a21", "a20", "a31", "x10", "a32", "a22", "s1", "a10", "j", "x21", "x22", "x20", "s0",
    "a11", "x32", "l", "a12", "x31", "x23", "x33", "p3", "g", "p2", "x11", "s2", "x12", "p0",
    "x13", "p1",
)
FIRST = (
    "b0", "b2", "s0", "b3", "b1", "s2", "s3", "k0", "s1", "k2", "z0", "z2", "h0", "k1",
    "k3", "h2", "z1", "f2", "z3", "h1", "f0", "m2", "h3", "r0", "f1", "m0", "e2", "f3",
    "m1", "a2", "m3", "e0", "e1", "a0", "a1", "e3", "a3",
)
SECOND = (
    "b2", "s2", "b0", "b3", "s0", "b1", "k2", "s1", "s3", "k0", "z2", "k1", "z0", "k3",
    "z1", "h0", "z3", "h1", "h2", "h3",
)


def halves(value):
    hi = value.astype(jnp.bfloat16)
    return hi, (value - hi.astype(jnp.float32)).astype(jnp.bfloat16)


def dot3(a, b, dims):
    dot = lambda u, v: lax.dot_general(u, v, dims, preferred_element_type=jnp.float32)
    return dot(a[0], b[0]) + (dot(a[0], b[1]) + dot(a[1], b[0]))


def fused(
    R, C, count,
    x_ref, ve_ref, ce_ref, pv_ref, pc_ref, w_ref,
    out_ref, coef_ref,
    ql, hl, pvl, pcl, il1, il2, bk, cr, yr, kb, xr, zr, sa, sb,
    pvt, pc3, xs, xh, it, wt, acc1, acc2, wtr, wv, q1, gap,
    w_s, qz_s, qz_r, qx_s, qx_r, vz_s, vz_r, vx_s, vx_r, cy_s, cy_r, cc_s, cc_r,
    jy_s, jy_r, jc_s, jc_r, iy_s, iy_r, ic_s, ic_r, gz_s, gz_r, gx_s, gx_r,
    cr_s, cr_r, yr_s, yr_r, xr_s, xr_r, zr_s, zr_r, sa_s, sa_r, sb_s, sb_r,
):
    NY, NZ = R // 2, C // 2
    r, c = lax.axis_index("row"), lax.axis_index("col")
    y, k, z, h = r // 2, r % 2, c // 2, c % 2
    nv, ncl = x_ref.shape
    np_, nvl = pv_ref.shape
    pcn, npc = pc_ref.shape
    m = nv // CHUNKS
    per = CHUNKS // 2
    pp = np_ // PIECES
    pending = []

    def copy(src, dst, ss, rs, dev):
        return pltpu.make_async_remote_copy(
            src_ref=src, dst_ref=dst, send_sem=ss, recv_sem=rs, device_id=dev, device_id_type=MESH
        )

    def send(src, dst, ss, rs, dev, when=None):
        args = (src, dst, ss, rs, dev)
        start = lambda: copy(*args).start()
        pl.when(when)(start) if when is not None else start()
        pending.append((when, args))

    def wait(dst, ss, rs):
        copy(dst, dst, ss, rs, (r, c)).wait_recv()

    zdev = lambda d: (r, ((z + d) % NZ) * 2 + h)
    zfrom = lambda d: (z - d + NZ) % NZ
    xpeer = (r, z * 2 + 1 - h)
    ydev = lambda d: (((y + d) % NY) * 2 + k, c)
    yfrom = lambda d: (y - d + NY) % NY
    kpeer = (y * 2 + 1 - k, c)
    near = [d for d in range(1, NZ) if d in (1, NZ - 1)] + [d for d in range(2, NZ - 1)]
    far = near[2:] + near[:2]

    load_w = pltpu.make_async_copy(w_ref, wv, w_s)
    load_w.start()
    barrier = pltpu.get_barrier_semaphore()
    for d in range(1, C):
        pl.semaphore_signal(barrier, inc=1, device_id=(r, (c + d) % C), device_id_type=MESH)
    for d in range(1, R):
        pl.semaphore_signal(barrier, inc=1, device_id=((r + d) % R, c), device_id_type=MESH)

    start = x_ref[...]
    ve = jnp.broadcast_to(ve_ref[...], (ncl, nv)).T
    gap[...] = ce_ref[...] - ve
    squares = start * start
    sums = [jnp.sum(squares), jnp.sum(squares * gap[...])]
    pl.semaphore_wait(barrier, C + R - 2)

    def reduce_start(i, values):
        rows = [jnp.broadcast_to(v.reshape(1, 1), (1, 128)) for v in values]
        rows += [jnp.zeros((1, 128), jnp.float32)] * (8 - len(rows))
        sa[i, c] = jnp.concatenate(rows, axis=0)
        for d in range(1, C):
            send(sa.at[i, c], sa.at[i, c], sa_s.at[i, d], sa_r.at[i, d], (r, (c + d) % C))

    def reduce_middle(i):
        for d in range(1, C):
            wait(sa.at[i, (c - d + C) % C], sa_s.at[i, d], sa_r.at[i, d])
        sb[i, r] = jnp.sum(sa[i], axis=0)
        for d in range(1, R):
            send(sb.at[i, r], sb.at[i, r], sb_s.at[i, d], sb_r.at[i, d], ((r + d) % R, c))

    def reduce_end(i):
        for d in range(1, R):
            wait(sb.at[i, (r - d + R) % R], sb_s.at[i, d], sb_r.at[i, d])
        total = jnp.sum(sb[i], axis=0)
        return [total[j : j + 1, 0:1] for j in range(3)]

    piece = lambda j: pl.ds(j * pp, pp)
    rows_of = lambda i: pl.ds(i * m, m)

    side = z // (NZ // 2)
    mirror = z + side * (NZ - 1 - 2 * z)

    def origin(n):
        o = n + (n + NZ - mirror) // NZ
        return o + side * (NZ - 1 - 2 * o)

    def zown(src, dst, ss, rs):
        for up in range(2):
            to = z + 2 * up - 1
            send(src, dst, ss.at[z, up], rs.at[z], (r, to * 2 + h), (to >= 0) & (to < NZ))

    def znext(o, slot, ss, rs):
        wait(slot, ss.at[o, 0], rs.at[o])
        up = (z - o - 1 + NZ) // NZ
        to = z + 2 * up - 1
        send(slot, slot, ss.at[o, 0], rs.at[o], (r, to * 2 + h), (to >= 0) & (to < NZ))

    def own_x(j):
        send(pv_ref.at[piece(j)], pvl.at[c, piece(j)], vx_s.at[j, z], vx_r.at[j, z], xpeer)

    def own_z(j):
        zown(pv_ref.at[piece(j)], pvl.at[c, piece(j)], vz_s.at[j, h], vz_r.at[j, h])

    zown(x_ref, ql.at[c], qz_s, qz_r)
    send(x_ref, ql.at[c], qx_s.at[z], qx_r.at[z], xpeer)
    for d in range(1, NY):
        send(pc_ref, pcl.at[r], cy_s.at[d], cy_r.at[d], ydev(d))
    send(pc_ref, pcl.at[r], cc_s.at[0], cc_r.at[0], kpeer)
    own_x(0)
    own_z(0)
    reduce_start(0, sums)

    def put_x(dst, t, rows, b, value):
        hi, lo = halves(value)
        dst[0, rows, b * ncl : (b + 1) * ncl] = hi
        dst[1, rows, b * ncl : (b + 1) * ncl] = lo

    def put_pc(b, value):
        hi, lo = halves(value)
        pc3[0, b] = hi
        pc3[1, b] = lo

    def put_pv(j, zz, hh, value):
        hi, lo = halves(value.T)
        for u in range(per):
            pvt[0, hh * per + u, zz, :, piece(j)] = hi[u * m : (u + 1) * m]
            pvt[1, hh * per + u, zz, :, piece(j)] = lo[u * m : (u + 1) * m]

    def first_rows(n):
        o = origin(n)
        slot = ql.at[o * 2 + h]
        znext(o, slot, qz_s, qz_r)
        send(slot, slot, qx_s.at[o], qx_r.at[o], xpeer)

    def shared_piece(n):
        o = origin(n)
        for hh in range(2):
            slot = pvl.at[o * 2 + hh, piece(0)]
            znext(o, slot, vz_s.at[0, hh], vz_r.at[0, hh])
            put_pv(0, o, hh, pvl[o * 2 + hh, piece(0), :])

    ql[c] = start
    put_pc(r, pc_ref[...])
    put_pv(0, z, h, pv_ref[piece(0), :])
    def image_of(ref, rows):
        total = None
        for b in range(R):
            cols = slice(b * npc, (b + 1) * npc)
            part = dot3((ref[0, rows, cols], ref[1, rows, cols]), (pc3[0, b], pc3[1, b]), NT)
            total = part if total is None else total + part
        return total

    def arrive(j, n):
        o = origin(n)
        slot = pvl.at[o * 2 + h, piece(j)]
        znext(o, slot, vz_s.at[j, h], vz_r.at[j, h])
        send(slot, slot, vx_s.at[j, o], vx_r.at[j, o], xpeer)
        put_pv(j, o, h, pvl[o * 2 + h, piece(j), :])

    def across(j, o):
        b = o * 2 + 1 - h
        wait(pvl.at[b, piece(j)], vx_s.at[j, o], vx_r.at[j, o])
        put_pv(j, o, 1 - h, pvl[b, piece(j), :])

    def points(j, scale):
        parts = [pvt[t, :, :, :, piece(j)].reshape(CHUNKS * R * m, pp) for t in range(2)]
        part = dot3((it[0], it[1]), parts, NN)
        acc1[:, piece(j)] = part
        wt[0, :, piece(j)], wt[1, :, piece(j)] = halves(part * scale * wtr[:, piece(j)])

    def flip(i, value):
        it[0, :, i * R * m : (i + 1) * R * m], it[1, :, i * R * m : (i + 1) * R * m] = halves(value.T)

    def first_image():
        for d in range(1, NY):
            slot = il1.at[yfrom(d) * 2 + k]
            wait(slot, jy_s.at[d], jy_r.at[d])
            send(slot, slot, jc_s.at[d], jc_r.at[d], kpeer)

    def flip_image():
        for d in range(NY):
            wait(il1.at[yfrom(d) * 2 + 1 - k], jc_s.at[d], jc_r.at[d])
        for i in range(CHUNKS):
            flip(i, jnp.concatenate([il1[b, rows_of(i), :] for b in range(R)], axis=0))

    def conduction():
        reduce_middle(0)
        wait(pcl.at[y * 2 + 1 - k], cc_s.at[0], cc_r.at[0])
        put_pc(y * 2 + 1 - k, pcl[y * 2 + 1 - k])
        for d in range(1, NY):
            slot = pcl.at[yfrom(d) * 2 + k]
            wait(slot, cy_s.at[d], cy_r.at[d])
            send(slot, slot, cc_s.at[d], cc_r.at[d], kpeer)
            put_pc(yfrom(d) * 2 + k, pcl[yfrom(d) * 2 + k])

    def send_image():
        for o in range(NZ):
            wait(ql.at[o * 2 + 1 - h], qx_s.at[o], qx_r.at[o])
        for b in range(C):
            put_x(xs, 0, slice(None), b, ql[b])
        for d in range(1, NY):
            b = yfrom(d) * 2 + 1 - k
            wait(pcl.at[b], cc_s.at[d], cc_r.at[d])
            put_pc(b, pcl[b])
        il1[r] = image_of(xs, slice(None))
        for d in range(1, NY):
            send(il1.at[r], il1.at[r], jy_s.at[d], jy_r.at[d], ydev(d))
        send(il1.at[r], il1.at[r], jc_s.at[0], jc_r.at[0], kpeer)

    def peer_piece():
        slot = pvl.at[z * 2 + 1 - h, piece(0)]
        wait(slot, vx_s.at[0, z], vx_r.at[0, z])
        zown(slot, slot, vz_s.at[0, 1 - h], vz_r.at[0, 1 - h])

    def peer_put():
        put_pv(0, z, 1 - h, pvl[z * 2 + 1 - h, piece(0), :])

    def flip_weights():
        load_w.wait()
        wtr[...] = wv[...].T

    def own_piece(j):
        own_z(j)
        put_pv(j, z, h, pv_ref[piece(j), :])

    def crossed(j, n):
        across(j, z if n == 0 else origin(n - 1))

    first = {}

    def normalise():
        total, gaps, _ = reduce_end(0)
        mean = total / count
        first["mean"] = mean
        first["scale"] = 1.0 / jnp.sqrt(mean + EPS)
        first["shift"] = (gaps / count) / (mean + EPS)

    def finish_piece(j):
        if not first:
            normalise()
        points(j, first["scale"])

    opening = dict(
        f=first_rows, q=peer_piece, g=peer_put, o=own_x, w=own_piece, s=shared_piece, a=arrive, x=crossed,
        t=flip_weights, c=conduction, i=send_image, j=first_image, l=flip_image, p=finish_piece,
    )
    for name in OPENING:
        opening[name[0]](*(int(v) for v in name[1:]))
    mean, scale, shift = first["mean"], first["scale"], first["shift"]
    q1[...] = start * scale
    gap[...] = gap[...] - shift

    zero = jnp.zeros((m, ncl), jnp.float32)
    sums = {0: [zero, zero], 1: [zero, zero, zero]}
    state = {}
    counts = [0, 0, 0]

    def back(s, i):
        lhs = [pvt[t, i].reshape(R * m, np_) for t in range(2)]
        part = dot3(lhs, (wt[0], wt[1]), NT)
        for b in range(R):
            bk[s, i, b % 2, b // 2] = part[b * m : (b + 1) * m]
        send(bk.at[s, i, 1 - k], cr.at[s, i], cr_s.at[s, i], cr_r.at[s, i], kpeer)

    def spread(s, i):
        wait(cr.at[s, i], cr_s.at[s, i], cr_r.at[s, i])
        for d in range(1, NY):
            yy = (y + d) % NY
            bk[s, i, k, yy] = bk[s, i, k, yy] + cr[s, i, yy]
            send(bk.at[s, i, k, yy], yr.at[s, i, d], yr_s.at[s, i, d], yr_r.at[s, i, d], ydev(d))

    def kernel_part(s, i):
        summed = bk[s, i, k, y] + cr[s, i, y]
        for d in range(1, NY):
            wait(yr.at[s, i, d], yr_s.at[s, i, d], yr_r.at[s, i, d])
            summed = summed + yr[s, i, d]
        flat = halves(summed)
        for b in range(R):
            part = dot3(flat, (pc3[0, b], pc3[1, b]), NN)
            for u in range(npc // ncl):
                at = b * (npc // ncl) + u
                kb[s, i, at % 2, at // 2] = part[:, u * ncl : (u + 1) * ncl]
        send(kb.at[s, i, 1 - h], xr.at[s, i], xr_s.at[s, i], xr_r.at[s, i], xpeer)

    def zsum(s, i):
        wait(xr.at[s, i], xr_s.at[s, i], xr_r.at[s, i])
        for d in far:
            zz = (z + d) % NZ
            kb[s, i, h, zz] = kb[s, i, h, zz] + xr[s, i, zz]
            send(kb.at[s, i, h, zz], zr.at[s, i, d], zr_s.at[s, i, d], zr_r.at[s, i, d], zdev(d))

    def vector_part(s, i):
        rows = rows_of(i)
        total = kb[s, i, h, z] + xr[s, i, z]
        for d in near:
            wait(zr.at[s, i, d], zr_s.at[s, i, d], zr_r.at[s, i, d])
            total = total + zr[s, i, d]
        before = q1[rows, :]
        if s == 0:
            image = gap[rows, :] * before - total
            hl[c, rows, :] = image
            own = hl.at[c, rows]
            for d in near:
                send(own, own, gz_s.at[i, d], gz_r.at[i, d], zdev(d))
            send(own, own, gx_s.at[i, 0], gx_r.at[i, 0], xpeer)
            sums[0][0] += before * image
            sums[0][1] += image * image
        else:
            vector = (hl[c, rows, :] - state["move"] * before) / state["beta"]
            image = gap[rows, :] * vector - total
            acc1[rows, :ncl] = vector
            acc1[rows, ncl : 2 * ncl] = image
            sums[1][0] += vector * image
            sums[1][1] += image * image
            sums[1][2] += before * image
        counts[s] += 1
        if counts[s] == CHUNKS:
            reduce_start(1 + s, [jnp.sum(v) for v in sums[s]])

    def forward(s, i):
        for d in near:
            slot = hl.at[zfrom(d) * 2 + h, rows_of(i)]
            wait(slot, gz_s.at[i, d], gz_r.at[i, d])
            send(slot, slot, gx_s.at[i, d], gx_r.at[i, d], xpeer)

    def image_part(s, i):
        rows = rows_of(i)
        for d in [0] + near:
            wait(hl.at[zfrom(d) * 2 + 1 - h, rows], gx_s.at[i, d], gx_r.at[i, d])
        for b in range(C):
            put_x(xh, 1, rows, b, hl[b, rows, :])
        il2[i, r] = image_of(xh, rows)
        own = il2.at[i, r]
        for d in range(1, NY):
            send(own, own, iy_s.at[i, d], iy_r.at[i, d], ydev(d))
        send(own, own, ic_s.at[i, 0], ic_r.at[i, 0], kpeer)

    def exchange(s, i):
        for d in range(1, NY):
            slot = il2.at[i, yfrom(d) * 2 + k]
            wait(slot, iy_s.at[i, d], iy_r.at[i, d])
            send(slot, slot, ic_s.at[i, d], ic_r.at[i, d], kpeer)

    def scalars(s, i):
        reduce_middle(1)

    def add_points(s, i):
        for d in range(NY):
            wait(il2.at[i, yfrom(d) * 2 + 1 - k], ic_s.at[i, d], ic_r.at[i, d])
        flip(i, il2[i].reshape(R * m, pcn))
        cols = slice(i * R * m, (i + 1) * R * m)
        counts[2] += 1
        last = counts[2] == CHUNKS
        if last:
            cross, square, _ = reduce_end(1)
            inside, norm = cross / count, mean / (mean + EPS)
            move = inside - shift * (EPS / (mean + EPS))
            beta = jnp.sqrt(square / count - 2.0 * move * inside + move * move * norm + EPS)
            state.update(move=move, beta=beta, norm=norm, alpha=shift + move)
            inverse, drop = 1.0 / beta, move * scale
        for j in range(PIECES):
            lanes = piece(j)
            rhs = [pvt[t, i, :, :, lanes].reshape(R * m, pp) for t in range(2)]
            part = dot3((it[0, :, cols], it[1, :, cols]), rhs, NN)
            if counts[2] > 1:
                part = acc2[:, lanes] + part
            if last:
                part = (part - drop * acc1[:, lanes]) * inverse * wtr[:, lanes]
                wt[0, :, lanes], wt[1, :, lanes] = halves(part)
            else:
                acc2[:, lanes] = part

    events = dict(
        b=back, s=spread, k=kernel_part, z=zsum, h=vector_part, f=forward,
        m=image_part, e=exchange, a=add_points, r=scalars,
    )
    for s, order in enumerate((FIRST, SECOND)):
        for name in order:
            events[name[0]](s, int(name[1:]))

    reduce_middle(2)
    cross, square, older = [v / count for v in reduce_end(2)]
    move, beta, norm, alpha = (state[n] for n in ("move", "beta", "norm", "alpha"))
    size = 1.0 - EPS / (beta * beta)
    overlap = (EPS / (mean + EPS)) * alpha / beta
    step = cross - shift * (EPS / (beta * beta))
    squared = (
        square + step * step * size + beta * beta * norm
        - 2.0 * step * cross - 2.0 * beta * older + 2.0 * step * beta * overlap
    )
    beta2 = jnp.sqrt(squared + EPS)
    vector, image = acc1[:nv, :ncl], acc1[:nv, ncl : 2 * ncl]
    out_ref[...] = (image - step * vector - beta * q1[...]) / beta2
    for j, value in enumerate((alpha, beta, shift + step, beta2)):
        coef_ref[j : j + 1, :] = jnp.broadcast_to(value, (1, 128))
    for when, args in pending:
        finish = lambda: copy(*args).wait_send()
        pl.when(when)(finish) if when is not None else finish()


def fused_shards(R, C, excitons, valence_energy, conduction_energy, psi_valence, psi_conduction, screened):
    nv, nc = excitons.shape
    pr, pcn = screened.shape
    nvl, npc = psi_valence.shape[1], psi_conduction.shape[1]
    f32, bf16 = jnp.float32, jnp.bfloat16
    NY, NZ = R // 2, C // 2
    n, m = CHUNKS, nv // CHUNKS
    vm, dma = pltpu.VMEM, pltpu.SemaphoreType.DMA
    count = float(NV * NC)
    scratch = [
        vm((C, nv, nc), f32), vm((C, nv, nc), f32), vm((C, pr, nvl), f32), vm((R, pcn, npc), f32),
        vm((R, nv, pcn), f32), vm((n, R, m, pcn), f32),
        vm((2, n, 2, NY, m, pcn), f32), vm((2, n, NY, m, pcn), f32), vm((2, n, NY, m, pcn), f32),
        vm((2, n, 2, NZ, m, nc), f32), vm((2, n, NZ, m, nc), f32), vm((2, n, NZ, m, nc), f32),
        vm((3, C, 8, 128), f32), vm((3, R, 8, 128), f32),
        vm((2, n, R, m, pr), bf16), vm((2, R, pcn, npc), bf16), vm((2, nv, NC), bf16), vm((2, nv, NC), bf16),
        vm((2, pcn, NV), bf16), vm((2, pcn, pr), bf16),
        vm((pcn, pr), f32), vm((pcn, pr), f32), vm((pcn, pr), f32), vm((pr, pcn), f32),
        vm((nv, nc), f32), vm((nv, nc), f32),
        dma(()),
    ]
    pairs = [
        [(NZ, 2), (NZ,)], (NZ,), [(PIECES, 2, NZ, 2), (PIECES, 2, NZ)], (PIECES, NZ), (NY,), (NY,), (NY,), (NY,), (n, NY), (n, NY), (n, NZ), (n, NZ),
        (2, n), (2, n, NY), (2, n), (2, n, NZ), (3, C), (3, R),
    ]
    for shape in pairs:
        both = shape if isinstance(shape, list) else [shape, shape]
        scratch += [dma(v) for v in both]
    vector, coef = pl.pallas_call(
        lambda *refs: fused(R, C, count, *refs),
        out_shape=(jax.ShapeDtypeStruct((nv, nc), f32), jax.ShapeDtypeStruct((4, 128), f32)),
        in_specs=[pl.BlockSpec(memory_space=vm)] * 5 + [pl.BlockSpec(memory_space=pl.ANY)],
        out_specs=(pl.BlockSpec(memory_space=vm), pl.BlockSpec(memory_space=vm)),
        scratch_shapes=scratch,
        compiler_params=pltpu.CompilerParams(collective_id=0, has_side_effects=True, vmem_limit_bytes=67043328),
    )(excitons, valence_energy.reshape(1, nv), conduction_energy.reshape(1, nc), psi_valence, psi_conduction, screened)
    return vector, coef[:, 0]


def solution(mesh):
    R, C = mesh.shape["row"], mesh.shape["col"]
    covered = max(int(v[1:]) for v in OPENING if v[0] == "f") == C // 2 - 2
    aligned = covered and C == 2 * R and R % 2 == 0 and STEPS == 2 and NV == NC and (NV // R) % (16 * CHUNKS) == 0 and (NV // R) % 128 == 0 and (NC // C) % 128 == 0
    body = (lambda *args: fused_shards(R, C, *args)) if aligned else shards
    return jax.shard_map(
        body,
        mesh=mesh,
        in_specs=(
            P("row", "col"),
            P("row"),
            P("col"),
            P("row", "col"),
            P("col", "row"),
            P("row", "col"),
        ),
        out_specs=(P("row", "col"), P()),
        check_vma=False,
    )
```

```python
import jax
import jax.numpy as jnp
from jax import lax
from jax.experimental import pallas as pl
from jax.experimental.pallas import tpu as pltpu
from jax.sharding import PartitionSpec as P

NV = 1024
NC = 1024
STEPS = 2


EPS = 1e-06


def shards(excitons, valence_energy, conduction_energy, psi_valence, psi_conduction, screened):
    high = lax.Precision.HIGHEST
    count = NV * NC
    energy_gap = conduction_energy[None, :] - valence_energy[:, None]
    total = lax.psum(jnp.sum(excitons * excitons), ("row", "col"))
    vector = excitons / jnp.sqrt(total / count + EPS)
    previous = jnp.zeros_like(vector)
    beta_prev = jnp.zeros((), jnp.float32)
    values = []
    for step in range(STEPS):
        panel_valence = lax.all_gather(psi_valence, "col", axis=1, tiled=True)
        panel_conduction = lax.all_gather(psi_conduction, "row", axis=1, tiled=True)
        full_rows = lax.all_gather(vector, "col", axis=1, tiled=True)
        image_block = jnp.dot(full_rows, panel_conduction.T, precision=high)
        image_columns = lax.all_gather(image_block, "row", axis=0, tiled=True)
        points = jnp.dot(panel_valence, image_columns, precision=high)
        weighted = points * screened
        back_valence = lax.psum_scatter(
            jnp.dot(panel_valence.T, weighted, precision=high),
            "row",
            scatter_dimension=0,
            tiled=True,
        )
        back_flipped = back_valence.T
        kernel_flipped = lax.psum_scatter(
            jnp.dot(panel_conduction.T, back_flipped, precision=high),
            "col",
            scatter_dimension=0,
            tiled=True,
        )
        image = energy_gap * vector - kernel_flipped.T
        cross, square, older = lax.psum(
            (jnp.sum(vector * image), jnp.sum(image * image), jnp.sum(previous * image)),
            ("row", "col"),
        )
        alpha = cross / count
        residual = image - alpha * vector - beta_prev * previous
        squared = (
            square / count - alpha * alpha - 2.0 * beta_prev * older / count + beta_prev * beta_prev
        )
        beta = jnp.sqrt(squared + EPS)
        previous = vector
        vector = residual / beta
        beta_prev = beta
        values.append(alpha)
        values.append(beta)
    return (vector, jnp.stack(values))


MESH = pl.DeviceIdType.MESH
NN = (((1,), (0,)), ((), ()))
NT = (((1,), (1,)), ((), ()))
CHUNKS = 8
GROUP = 2
PIECES = 4
OPENING = (
    "t", "f0", "f1", "o2", "w3", "f2", "w2", "w1", "q", "o3", "a30", "c", "o1", "i",
    "x30", "a21", "a20", "a31", "x10", "a32", "a22", "s1", "a10", "j", "x21", "x22", "x20", "s0",
    "a11", "x32", "l", "a12", "x31", "x23", "x33", "p3", "g", "p2", "x11", "s2", "x12", "p0",
    "x13", "p1",
)
FIRST = (
    "b3", "b0", "s7", "b1", "s6", "s2", "s0", "k7", "b2", "k6", "s1", "s4", "k2", "z7",
    "k0", "z6", "k1", "z2", "s3", "k4", "s5", "z0", "h7", "z1", "z4", "k3", "k5", "h6",
    "h0", "z5", "f7", "f6", "h4", "z3", "h2", "f0", "h1", "h5", "m6", "m7", "f4", "m0",
    "f2", "h3", "f1", "m4", "f5", "m2", "e0", "e6", "f3", "m1", "e7", "r0", "m5", "m3",
    "e1", "e2", "a3", "e4", "e5", "a0", "e3", "a2", "a1",
)
SECOND = (
    "b0", "b1", "s0", "b3", "s3", "b2", "s2", "k0", "s7", "s6", "k3", "k2", "s1", "s4",
    "s5", "z0", "k7", "z3", "k6", "z2", "k1", "z7", "k4", "z6", "k5", "z1", "z4", "z5",
    "h6", "h1", "h0", "h3", "h4", "h2", "h7", "h5",
)


def halves(value):
    hi = value.astype(jnp.bfloat16)
    return hi, (value - hi.astype(jnp.float32)).astype(jnp.bfloat16)


def dot3(a, b, dims):
    dot = lambda u, v: lax.dot_general(u, v, dims, preferred_element_type=jnp.float32)
    return dot(a[0], b[0]) + (dot(a[0], b[1]) + dot(a[1], b[0]))


def fused(
    R, C, count,
    x_ref, ve_ref, ce_ref, pv_ref, pc_ref, w_ref,
    out_ref, coef_ref,
    ql, hl, pvl, pcl, il1, il2, bk, cr, yr, kb, xr, zr, sa, sb, sc,
    pvt, pc3, xs, xh, it, wt, acc1, acc2, wtr, wv, q1, gap,
    w_s, qz_s, qz_r, qx_s, qx_r, vz_s, vz_r, vx_s, vx_r, cy_s, cy_r, cc_s, cc_r,
    jy_s, jy_r, jc_s, jc_r, iy_s, iy_r, ic_s, ic_r, gz_s, gz_r, gx_s, gx_r,
    cr_s, cr_r, yr_s, yr_r, xr_s, xr_r, zr_s, zr_r, sa_s, sa_r, sb_s, sb_r, sc_s, sc_r,
):
    NY, NZ = R // 2, C // 2
    r, c = lax.axis_index("row"), lax.axis_index("col")
    y, k, z, h = r // 2, r % 2, c // 2, c % 2
    nv, ncl = x_ref.shape
    np_, nvl = pv_ref.shape
    pcn, npc = pc_ref.shape
    m = nv // CHUNKS
    per = CHUNKS // 2
    pp = np_ // PIECES
    pending = []

    def copy(src, dst, ss, rs, dev):
        return pltpu.make_async_remote_copy(
            src_ref=src, dst_ref=dst, send_sem=ss, recv_sem=rs, device_id=dev, device_id_type=MESH
        )

    def send(src, dst, ss, rs, dev, when=None):
        args = (src, dst, ss, rs, dev)
        start = lambda: copy(*args).start()
        pl.when(when)(start) if when is not None else start()
        pending.append((when, args))

    def wait(dst, ss, rs):
        copy(dst, dst, ss, rs, (r, c)).wait_recv()

    zdev = lambda d: (r, ((z + d) % NZ) * 2 + h)
    zfrom = lambda d: (z - d + NZ) % NZ
    xpeer = (r, z * 2 + 1 - h)
    ydev = lambda d: (((y + d) % NY) * 2 + k, c)
    yfrom = lambda d: (y - d + NY) % NY
    kpeer = (y * 2 + 1 - k, c)
    near = [d for d in range(1, NZ) if d in (1, NZ - 1)] + [d for d in range(2, NZ - 1)]
    far = near[2:] + near[:2]

    load_w = pltpu.make_async_copy(w_ref, wv, w_s)
    load_w.start()
    barrier = pltpu.get_barrier_semaphore()
    for d in range(1, R * C):
        at = (r * C + c + d) % (R * C)
        pl.semaphore_signal(barrier, inc=1, device_id=(at // C, at % C), device_id_type=MESH)

    start = x_ref[...]
    ve = jnp.broadcast_to(ve_ref[...], (ncl, nv)).T
    gap[...] = ce_ref[...] - ve
    squares = start * start
    sums = [jnp.sum(squares), jnp.sum(squares * gap[...])]
    pl.semaphore_wait(barrier, R * C - 1)

    def reduce_start(i, values):
        rows = [jnp.broadcast_to(v.reshape(1, 1), (1, 128)) for v in values]
        rows += [jnp.zeros((1, 128), jnp.float32)] * (8 - len(rows))
        sa[i, c] = jnp.concatenate(rows, axis=0)
        for d in range(1, C):
            send(sa.at[i, c], sa.at[i, c], sa_s.at[i, d], sa_r.at[i, d], (r, (c + d) % C))

    def reduce_middle(i):
        for d in range(1, C):
            wait(sa.at[i, (c - d + C) % C], sa_s.at[i, d], sa_r.at[i, d])
        sb[i, r] = jnp.sum(sa[i], axis=0)
        for d in range(1, R):
            send(sb.at[i, r], sb.at[i, r], sb_s.at[i, d], sb_r.at[i, d], ((r + d) % R, c))

    others = range(1, R * C)

    def place(d):
        at = (r * C + c + d) % (R * C)
        return at // C, at % C

    def whole_start(values):
        rows = [jnp.broadcast_to(v.reshape(1, 1), (1, 128)) for v in values]
        rows += [jnp.zeros((1, 128), jnp.float32)] * (8 - len(rows))
        sc[r * C + c] = jnp.concatenate(rows, axis=0)
        for d in others:
            send(sc.at[r * C + c], sc.at[r * C + c], sc_s.at[d], sc_r.at[d], place(d))

    def whole_end():
        for d in others:
            wait(sc.at[(r * C + c + R * C - d) % (R * C)], sc_s.at[d], sc_r.at[d])
        total = jnp.sum(sc[...], axis=0)
        return [total[j : j + 1, 0:1] for j in range(3)]

    def reduce_end(i):
        for d in range(1, R):
            wait(sb.at[i, (r - d + R) % R], sb_s.at[i, d], sb_r.at[i, d])
        total = jnp.sum(sb[i], axis=0)
        return [total[j : j + 1, 0:1] for j in range(3)]

    piece = lambda j: pl.ds(j * pp, pp)
    rows_of = lambda i: pl.ds(i * m, m)

    side = z // (NZ // 2)
    mirror = z + side * (NZ - 1 - 2 * z)

    def origin(n):
        o = n + (n + NZ - mirror) // NZ
        return o + side * (NZ - 1 - 2 * o)

    def zown(src, dst, ss, rs):
        for up in range(2):
            to = z + 2 * up - 1
            send(src, dst, ss.at[z, up], rs.at[z], (r, to * 2 + h), (to >= 0) & (to < NZ))

    def znext(o, slot, ss, rs):
        wait(slot, ss.at[o, 0], rs.at[o])
        up = (z - o - 1 + NZ) // NZ
        to = z + 2 * up - 1
        send(slot, slot, ss.at[o, 0], rs.at[o], (r, to * 2 + h), (to >= 0) & (to < NZ))

    def own_x(j):
        send(pv_ref.at[piece(j)], pvl.at[c, piece(j)], vx_s.at[j, z], vx_r.at[j, z], xpeer)

    def own_z(j):
        zown(pv_ref.at[piece(j)], pvl.at[c, piece(j)], vz_s.at[j, h], vz_r.at[j, h])

    zown(x_ref, ql.at[c], qz_s, qz_r)
    send(x_ref, ql.at[c], qx_s.at[z], qx_r.at[z], xpeer)
    for d in range(1, NY):
        send(pc_ref, pcl.at[r], cy_s.at[d], cy_r.at[d], ydev(d))
    send(pc_ref, pcl.at[r], cc_s.at[0], cc_r.at[0], kpeer)
    own_x(0)
    own_z(0)
    reduce_start(0, sums)

    def put_x(dst, t, rows, b, value):
        hi, lo = halves(value)
        dst[0, rows, b * ncl : (b + 1) * ncl] = hi
        dst[1, rows, b * ncl : (b + 1) * ncl] = lo

    def put_pc(b, value):
        hi, lo = halves(value)
        pc3[0, b] = hi
        pc3[1, b] = lo

    def put_pv(j, zz, hh, value):
        hi, lo = halves(value.T)
        for u in range(per):
            pvt[0, hh * per + u, zz, :, piece(j)] = hi[u * m : (u + 1) * m]
            pvt[1, hh * per + u, zz, :, piece(j)] = lo[u * m : (u + 1) * m]

    def first_rows(n):
        o = origin(n)
        slot = ql.at[o * 2 + h]
        znext(o, slot, qz_s, qz_r)
        send(slot, slot, qx_s.at[o], qx_r.at[o], xpeer)

    def shared_piece(n):
        o = origin(n)
        for hh in range(2):
            slot = pvl.at[o * 2 + hh, piece(0)]
            znext(o, slot, vz_s.at[0, hh], vz_r.at[0, hh])
            put_pv(0, o, hh, pvl[o * 2 + hh, piece(0), :])

    ql[c] = start
    put_pc(r, pc_ref[...])
    put_pv(0, z, h, pv_ref[piece(0), :])
    def image_of(ref, rows):
        total = None
        for b in range(R):
            cols = slice(b * npc, (b + 1) * npc)
            part = dot3((ref[0, rows, cols], ref[1, rows, cols]), (pc3[0, b], pc3[1, b]), NT)
            total = part if total is None else total + part
        return total

    def arrive(j, n):
        o = origin(n)
        slot = pvl.at[o * 2 + h, piece(j)]
        znext(o, slot, vz_s.at[j, h], vz_r.at[j, h])
        send(slot, slot, vx_s.at[j, o], vx_r.at[j, o], xpeer)
        put_pv(j, o, h, pvl[o * 2 + h, piece(j), :])

    def across(j, o):
        b = o * 2 + 1 - h
        wait(pvl.at[b, piece(j)], vx_s.at[j, o], vx_r.at[j, o])
        put_pv(j, o, 1 - h, pvl[b, piece(j), :])

    def points(j, scale):
        parts = [pvt[t, :, :, :, piece(j)].reshape(CHUNKS * R * m, pp) for t in range(2)]
        part = dot3((it[0], it[1]), parts, NN)
        acc1[:, piece(j)] = part
        wt[0, :, piece(j)], wt[1, :, piece(j)] = halves(part * scale * wtr[:, piece(j)])

    def flip(i, value):
        it[0, :, i * R * m : (i + 1) * R * m], it[1, :, i * R * m : (i + 1) * R * m] = halves(value.T)

    def first_image():
        for d in range(1, NY):
            slot = il1.at[yfrom(d) * 2 + k]
            wait(slot, jy_s.at[d], jy_r.at[d])
            send(slot, slot, jc_s.at[d], jc_r.at[d], kpeer)

    def flip_image():
        for d in range(NY):
            wait(il1.at[yfrom(d) * 2 + 1 - k], jc_s.at[d], jc_r.at[d])
        for i in range(CHUNKS):
            flip(i, jnp.concatenate([il1[b, rows_of(i), :] for b in range(R)], axis=0))

    def conduction():
        reduce_middle(0)
        wait(pcl.at[y * 2 + 1 - k], cc_s.at[0], cc_r.at[0])
        put_pc(y * 2 + 1 - k, pcl[y * 2 + 1 - k])
        for d in range(1, NY):
            slot = pcl.at[yfrom(d) * 2 + k]
            wait(slot, cy_s.at[d], cy_r.at[d])
            send(slot, slot, cc_s.at[d], cc_r.at[d], kpeer)
            put_pc(yfrom(d) * 2 + k, pcl[yfrom(d) * 2 + k])

    def send_image():
        for o in range(NZ):
            wait(ql.at[o * 2 + 1 - h], qx_s.at[o], qx_r.at[o])
        for b in range(C):
            put_x(xs, 0, slice(None), b, ql[b])
        for d in range(1, NY):
            b = yfrom(d) * 2 + 1 - k
            wait(pcl.at[b], cc_s.at[d], cc_r.at[d])
            put_pc(b, pcl[b])
        il1[r] = image_of(xs, slice(None))
        for d in range(1, NY):
            send(il1.at[r], il1.at[r], jy_s.at[d], jy_r.at[d], ydev(d))
        send(il1.at[r], il1.at[r], jc_s.at[0], jc_r.at[0], kpeer)

    def peer_piece():
        slot = pvl.at[z * 2 + 1 - h, piece(0)]
        wait(slot, vx_s.at[0, z], vx_r.at[0, z])
        zown(slot, slot, vz_s.at[0, 1 - h], vz_r.at[0, 1 - h])

    def peer_put():
        put_pv(0, z, 1 - h, pvl[z * 2 + 1 - h, piece(0), :])

    def flip_weights():
        load_w.wait()
        wtr[...] = wv[...].T

    def own_piece(j):
        own_z(j)
        put_pv(j, z, h, pv_ref[piece(j), :])

    def crossed(j, n):
        across(j, z if n == 0 else origin(n - 1))

    first = {}

    def normalise():
        total, gaps, _ = reduce_end(0)
        mean = total / count
        first["mean"] = mean
        first["scale"] = 1.0 / jnp.sqrt(mean + EPS)
        first["shift"] = (gaps / count) / (mean + EPS)

    def finish_piece(j):
        if not first:
            normalise()
        points(j, first["scale"])

    opening = dict(
        f=first_rows, q=peer_piece, g=peer_put, o=own_x, w=own_piece, s=shared_piece, a=arrive, x=crossed,
        t=flip_weights, c=conduction, i=send_image, j=first_image, l=flip_image, p=finish_piece,
    )
    for name in OPENING:
        opening[name[0]](*(int(v) for v in name[1:]))
    mean, scale, shift = first["mean"], first["scale"], first["shift"]
    q1[...] = start * scale
    gap[...] = gap[...] - shift

    zero = jnp.zeros((m, ncl), jnp.float32)
    sums = {0: [zero, zero], 1: [zero, zero, zero]}
    state = {}
    counts = [0, 0, 0]

    group = lambda g: range(g * GROUP, (g + 1) * GROUP)

    def back(s, g):
        lhs = [pvt[t, g * GROUP : (g + 1) * GROUP].reshape(GROUP * R * m, np_) for t in range(2)]
        part = dot3(lhs, (wt[0], wt[1]), NT)
        for u, i in enumerate(group(g)):
            for b in range(R):
                at = (u * R + b) * m
                bk[s, i, b % 2, b // 2] = part[at : at + m]
            send(bk.at[s, i, 1 - k], cr.at[s, i], cr_s.at[s, i], cr_r.at[s, i], kpeer)

    def spread(s, i):
        wait(cr.at[s, i], cr_s.at[s, i], cr_r.at[s, i])
        for d in range(1, NY):
            yy = (y + d) % NY
            bk[s, i, k, yy] = bk[s, i, k, yy] + cr[s, i, yy]
            send(bk.at[s, i, k, yy], yr.at[s, i, d], yr_s.at[s, i, d], yr_r.at[s, i, d], ydev(d))

    def kernel_part(s, i):
        summed = bk[s, i, k, y] + cr[s, i, y]
        for d in range(1, NY):
            wait(yr.at[s, i, d], yr_s.at[s, i, d], yr_r.at[s, i, d])
            summed = summed + yr[s, i, d]
        flat = halves(summed)
        for b in range(R):
            part = dot3(flat, (pc3[0, b], pc3[1, b]), NN)
            for u in range(npc // ncl):
                at = b * (npc // ncl) + u
                kb[s, i, at % 2, at // 2] = part[:, u * ncl : (u + 1) * ncl]
        send(kb.at[s, i, 1 - h], xr.at[s, i], xr_s.at[s, i], xr_r.at[s, i], xpeer)

    def zsum(s, i):
        wait(xr.at[s, i], xr_s.at[s, i], xr_r.at[s, i])
        for d in far:
            zz = (z + d) % NZ
            kb[s, i, h, zz] = kb[s, i, h, zz] + xr[s, i, zz]
            send(kb.at[s, i, h, zz], zr.at[s, i, d], zr_s.at[s, i, d], zr_r.at[s, i, d], zdev(d))

    def vector_part(s, i):
        rows = rows_of(i)
        total = kb[s, i, h, z] + xr[s, i, z]
        for d in near:
            wait(zr.at[s, i, d], zr_s.at[s, i, d], zr_r.at[s, i, d])
            total = total + zr[s, i, d]
        before = q1[rows, :]
        if s == 0:
            image = gap[rows, :] * before - total
            hl[c, rows, :] = image
            own = hl.at[c, rows]
            for d in near:
                send(own, own, gz_s.at[i, d], gz_r.at[i, d], zdev(d))
            send(own, own, gx_s.at[i, 0], gx_r.at[i, 0], xpeer)
            sums[0][0] += before * image
            sums[0][1] += image * image
        else:
            vector = (hl[c, rows, :] - state["move"] * before) / state["beta"]
            image = gap[rows, :] * vector - total
            acc1[rows, :ncl] = vector
            acc1[rows, ncl : 2 * ncl] = image
            sums[1][0] += vector * image
            sums[1][1] += image * image
            sums[1][2] += before * image
        counts[s] += 1
        if counts[s] == CHUNKS:
            partial = [jnp.sum(v) for v in sums[s]]
            reduce_start(1, partial) if s == 0 else whole_start(partial)

    def forward(s, i):
        for d in near:
            slot = hl.at[zfrom(d) * 2 + h, rows_of(i)]
            wait(slot, gz_s.at[i, d], gz_r.at[i, d])
            send(slot, slot, gx_s.at[i, d], gx_r.at[i, d], xpeer)

    def image_part(s, i):
        rows = rows_of(i)
        for d in [0] + near:
            wait(hl.at[zfrom(d) * 2 + 1 - h, rows], gx_s.at[i, d], gx_r.at[i, d])
        for b in range(C):
            put_x(xh, 1, rows, b, hl[b, rows, :])
        il2[i, r] = image_of(xh, rows)
        own = il2.at[i, r]
        for d in range(1, NY):
            send(own, own, iy_s.at[i, d], iy_r.at[i, d], ydev(d))
        send(own, own, ic_s.at[i, 0], ic_r.at[i, 0], kpeer)

    def exchange(s, i):
        for d in range(1, NY):
            slot = il2.at[i, yfrom(d) * 2 + k]
            wait(slot, iy_s.at[i, d], iy_r.at[i, d])
            send(slot, slot, ic_s.at[i, d], ic_r.at[i, d], kpeer)

    def scalars(s, i):
        reduce_middle(1)

    def add_points(s, g):
        for i in group(g):
            for d in range(NY):
                wait(il2.at[i, yfrom(d) * 2 + 1 - k], ic_s.at[i, d], ic_r.at[i, d])
            flip(i, il2[i].reshape(R * m, pcn))
        cols = slice(g * GROUP * R * m, (g + 1) * GROUP * R * m)
        counts[2] += 1
        last = counts[2] == CHUNKS // GROUP
        if last:
            cross, square, _ = reduce_end(1)
            inside, norm = cross / count, mean / (mean + EPS)
            move = inside - shift * (EPS / (mean + EPS))
            beta = jnp.sqrt(square / count - 2.0 * move * inside + move * move * norm + EPS)
            state.update(move=move, beta=beta, norm=norm, alpha=shift + move)
            inverse, drop = 1.0 / beta, move * scale
        for j in range(PIECES):
            lanes = piece(j)
            rhs = [pvt[t, g * GROUP : (g + 1) * GROUP, :, :, lanes].reshape(GROUP * R * m, pp) for t in range(2)]
            part = dot3((it[0, :, cols], it[1, :, cols]), rhs, NN)
            if counts[2] > 1:
                part = acc2[:, lanes] + part
            if last:
                part = (part - drop * acc1[:, lanes]) * inverse * wtr[:, lanes]
                wt[0, :, lanes], wt[1, :, lanes] = halves(part)
            else:
                acc2[:, lanes] = part

    events = dict(
        b=back, s=spread, k=kernel_part, z=zsum, h=vector_part, f=forward,
        m=image_part, e=exchange, a=add_points, r=scalars,
    )
    for s, order in enumerate((FIRST, SECOND)):
        for name in order:
            events[name[0]](s, int(name[1:]))

    cross, square, older = [v / count for v in whole_end()]
    move, beta, norm, alpha = (state[n] for n in ("move", "beta", "norm", "alpha"))
    size = 1.0 - EPS / (beta * beta)
    overlap = (EPS / (mean + EPS)) * alpha / beta
    step = cross - shift * (EPS / (beta * beta))
    squared = (
        square + step * step * size + beta * beta * norm
        - 2.0 * step * cross - 2.0 * beta * older + 2.0 * step * beta * overlap
    )
    beta2 = jnp.sqrt(squared + EPS)
    vector, image = acc1[:nv, :ncl], acc1[:nv, ncl : 2 * ncl]
    out_ref[...] = (image - step * vector - beta * q1[...]) / beta2
    for j, value in enumerate((alpha, beta, shift + step, beta2)):
        coef_ref[j] = value[0, 0]
    for when, args in pending:
        finish = lambda: copy(*args).wait_send()
        pl.when(when)(finish) if when is not None else finish()


def fused_shards(R, C, excitons, valence_energy, conduction_energy, psi_valence, psi_conduction, screened):
    nv, nc = excitons.shape
    pr, pcn = screened.shape
    nvl, npc = psi_valence.shape[1], psi_conduction.shape[1]
    f32, bf16 = jnp.float32, jnp.bfloat16
    NY, NZ = R // 2, C // 2
    n, m = CHUNKS, nv // CHUNKS
    vm, dma = pltpu.VMEM, pltpu.SemaphoreType.DMA
    count = float(NV * NC)
    scratch = [
        vm((C, nv, nc), f32), vm((C, nv, nc), f32), vm((C, pr, nvl), f32), vm((R, pcn, npc), f32),
        vm((R, nv, pcn), f32), vm((n, R, m, pcn), f32),
        vm((2, n, 2, NY, m, pcn), f32), vm((2, n, NY, m, pcn), f32), vm((2, n, NY, m, pcn), f32),
        vm((2, n, 2, NZ, m, nc), f32), vm((2, n, NZ, m, nc), f32), vm((2, n, NZ, m, nc), f32),
        vm((2, C, 8, 128), f32), vm((2, R, 8, 128), f32), vm((R * C, 8, 128), f32),
        vm((2, n, R, m, pr), bf16), vm((2, R, pcn, npc), bf16), vm((2, nv, NC), bf16), vm((2, nv, NC), bf16),
        vm((2, pcn, NV), bf16), vm((2, pcn, pr), bf16),
        vm((pcn, pr), f32), vm((pcn, pr), f32), vm((pcn, pr), f32), vm((pr, pcn), f32),
        vm((nv, nc), f32), vm((nv, nc), f32),
        dma(()),
    ]
    pairs = [
        [(NZ, 2), (NZ,)], (NZ,), [(PIECES, 2, NZ, 2), (PIECES, 2, NZ)], (PIECES, NZ), (NY,), (NY,), (NY,), (NY,), (n, NY), (n, NY), (n, NZ), (n, NZ),
        (2, n), (2, n, NY), (2, n), (2, n, NZ), (2, C), (2, R), (R * C,),
    ]
    for shape in pairs:
        both = shape if isinstance(shape, list) else [shape, shape]
        scratch += [dma(v) for v in both]
    vector, coef = pl.pallas_call(
        lambda *refs: fused(R, C, count, *refs),
        out_shape=(jax.ShapeDtypeStruct((nv, nc), f32), jax.ShapeDtypeStruct((4,), f32)),
        in_specs=[pl.BlockSpec(memory_space=vm)] * 5 + [pl.BlockSpec(memory_space=pl.ANY)],
        out_specs=(pl.BlockSpec(memory_space=vm), pl.BlockSpec(memory_space=pltpu.SMEM)),
        scratch_shapes=scratch,
        compiler_params=pltpu.CompilerParams(collective_id=0, has_side_effects=True, vmem_limit_bytes=67043328),
    )(excitons, valence_energy.reshape(1, nv), conduction_energy.reshape(1, nc), psi_valence, psi_conduction, screened)
    return vector, coef


def solution(mesh):
    R, C = mesh.shape["row"], mesh.shape["col"]
    covered = max(int(v[1:]) for v in OPENING if v[0] == "f") == C // 2 - 2
    aligned = covered and C == 2 * R and R % 2 == 0 and STEPS == 2 and NV == NC and (NV // R) % (16 * CHUNKS) == 0 and (NV // R) % 128 == 0 and (NC // C) % 128 == 0
    body = (lambda *args: fused_shards(R, C, *args)) if aligned else shards
    return jax.shard_map(
        body,
        mesh=mesh,
        in_specs=(
            P("row", "col"),
            P("row"),
            P("col"),
            P("row", "col"),
            P("col", "row"),
            P("row", "col"),
        ),
        out_specs=(P("row", "col"), P()),
        check_vma=False,
    )
```

```python
import jax
import jax.numpy as jnp
from jax import lax
from jax.experimental import pallas as pl
from jax.experimental.pallas import tpu as pltpu
from jax.sharding import PartitionSpec as P

NV = 1024
NC = 1024
STEPS = 2


EPS = 1e-06


def shards(excitons, valence_energy, conduction_energy, psi_valence, psi_conduction, screened):
    high = lax.Precision.HIGHEST
    count = NV * NC
    energy_gap = conduction_energy[None, :] - valence_energy[:, None]
    total = lax.psum(jnp.sum(excitons * excitons), ("row", "col"))
    vector = excitons / jnp.sqrt(total / count + EPS)
    previous = jnp.zeros_like(vector)
    beta_prev = jnp.zeros((), jnp.float32)
    values = []
    for step in range(STEPS):
        panel_valence = lax.all_gather(psi_valence, "col", axis=1, tiled=True)
        panel_conduction = lax.all_gather(psi_conduction, "row", axis=1, tiled=True)
        full_rows = lax.all_gather(vector, "col", axis=1, tiled=True)
        image_block = jnp.dot(full_rows, panel_conduction.T, precision=high)
        image_columns = lax.all_gather(image_block, "row", axis=0, tiled=True)
        points = jnp.dot(panel_valence, image_columns, precision=high)
        weighted = points * screened
        back_valence = lax.psum_scatter(
            jnp.dot(panel_valence.T, weighted, precision=high),
            "row",
            scatter_dimension=0,
            tiled=True,
        )
        back_flipped = back_valence.T
        kernel_flipped = lax.psum_scatter(
            jnp.dot(panel_conduction.T, back_flipped, precision=high),
            "col",
            scatter_dimension=0,
            tiled=True,
        )
        image = energy_gap * vector - kernel_flipped.T
        cross, square, older = lax.psum(
            (jnp.sum(vector * image), jnp.sum(image * image), jnp.sum(previous * image)),
            ("row", "col"),
        )
        alpha = cross / count
        residual = image - alpha * vector - beta_prev * previous
        squared = (
            square / count - alpha * alpha - 2.0 * beta_prev * older / count + beta_prev * beta_prev
        )
        beta = jnp.sqrt(squared + EPS)
        previous = vector
        vector = residual / beta
        beta_prev = beta
        values.append(alpha)
        values.append(beta)
    return (vector, jnp.stack(values))


MESH = pl.DeviceIdType.MESH
NN = (((1,), (0,)), ((), ()))
NT = (((1,), (1,)), ((), ()))
CHUNKS = 8
GROUP = 2
PIECES = 4
OPENING = (
    "o2", "t", "o3", "w3", "f0", "w2", "w1", "f1", "f2", "a10", "a21", "a20", "a12", "u",
    "o1", "c", "a22", "i", "x20", "x22", "a11", "q", "a30", "s1", "j", "x23", "x21", "s0",
    "a31", "g", "x11", "l", "x10", "x12", "a32", "x13", "x30", "p1", "p2", "x31", "s2", "x32",
    "p0", "x33", "p3",
)
FIRST = (
    "b3", "b0", "s7", "b1", "s6", "s2", "s0", "k7", "b2", "k6", "s1", "s4", "k2", "z7",
    "k0", "z6", "k1", "z2", "s3", "k4", "s5", "z0", "h7", "z1", "z4", "k3", "k5", "h6",
    "h0", "z5", "f7", "f6", "h4", "z3", "h2", "f0", "h1", "h5", "m6", "m7", "f4", "m0",
    "f2", "h3", "f1", "m4", "f5", "m2", "e0", "e6", "f3", "m1", "e7", "r0", "m5", "m3",
    "e1", "e2", "a3", "e4", "e5", "a0", "e3", "a2", "a1",
)
SECOND = (
    "b0", "b1", "s0", "b3", "s3", "b2", "s2", "k0", "s7", "s6", "k3", "k2", "s1", "s4",
    "s5", "z0", "k7", "z3", "k6", "z2", "k1", "z7", "k4", "z6", "k5", "z1", "z4", "z5",
    "h6", "h1", "h0", "h3", "h4", "h2", "h7", "h5",
)


def halves(value):
    hi = value.astype(jnp.bfloat16)
    return hi, (value - hi.astype(jnp.float32)).astype(jnp.bfloat16)


def dot3(a, b, dims):
    dot = lambda u, v: lax.dot_general(u, v, dims, preferred_element_type=jnp.float32)
    return dot(a[0], b[0]) + (dot(a[0], b[1]) + dot(a[1], b[0]))


def fused(
    R, C, count,
    x_in, ve_in, ce_in, pv_in, pc_in, w_ref,
    out_ref, coef_ref,
    ql, hl, pvl, pcl, il1, il2, bk, cr, yr, kb, xr, zr, sa, sb, sc,
    pvt, pc3, xs, xh, it, wt, acc1, acc2, wtr, wv, q1, gap,
    x_ref, ve_ref, ce_ref, pv_ref, pc_ref, w_s, in_s, qz_s, qz_r, qx_s, qx_r, vz_s, vz_r, vx_s, vx_r, cy_s, cy_r, cc_s, cc_r,
    jy_s, jy_r, jc_s, jc_r, iy_s, iy_r, ic_s, ic_r, gz_s, gz_r, gx_s, gx_r,
    cr_s, cr_r, yr_s, yr_r, xr_s, xr_r, zr_s, zr_r, sa_s, sa_r, sb_s, sb_r, sc_s, sc_r,
):
    NY, NZ = R // 2, C // 2
    r, c = lax.axis_index("row"), lax.axis_index("col")
    y, k, z, h = r // 2, r % 2, c // 2, c % 2
    nv, ncl = x_ref.shape
    np_, nvl = pv_ref.shape
    pcn, npc = pc_ref.shape
    m = nv // CHUNKS
    per = CHUNKS // 2
    pp = np_ // PIECES
    pending = []

    def copy(src, dst, ss, rs, dev):
        return pltpu.make_async_remote_copy(
            src_ref=src, dst_ref=dst, send_sem=ss, recv_sem=rs, device_id=dev, device_id_type=MESH
        )

    def send(src, dst, ss, rs, dev, when=None):
        args = (src, dst, ss, rs, dev)
        start = lambda: copy(*args).start()
        pl.when(when)(start) if when is not None else start()
        pending.append((when, args))

    def wait(dst, ss, rs):
        copy(dst, dst, ss, rs, (r, c)).wait_recv()

    zdev = lambda d: (r, ((z + d) % NZ) * 2 + h)
    zfrom = lambda d: (z - d + NZ) % NZ
    xpeer = (r, z * 2 + 1 - h)
    ydev = lambda d: (((y + d) % NY) * 2 + k, c)
    yfrom = lambda d: (y - d + NY) % NY
    kpeer = (y * 2 + 1 - k, c)
    near = [d for d in range(1, NZ) if d in (1, NZ - 1)] + [d for d in range(2, NZ - 1)]
    far = near[2:] + near[:2]

    loads = [
        pltpu.make_async_copy(src, dst, in_s.at[j])
        for j, (src, dst) in enumerate(
            ((x_in, x_ref), (ve_in, ve_ref), (ce_in, ce_ref), (pv_in, pv_ref), (pc_in, pc_ref))
        )
    ]
    load_w = pltpu.make_async_copy(w_ref, wv, w_s)
    for load in loads + [load_w]:
        load.start()
    barrier = pltpu.get_barrier_semaphore()
    for d in range(1, R * C):
        at = (r * C + c + d) % (R * C)
        pl.semaphore_signal(barrier, inc=1, device_id=(at // C, at % C), device_id_type=MESH)

    for load in loads[:3]:
        load.wait()
    start = x_ref[...]
    ve = jnp.broadcast_to(ve_ref[...], (ncl, nv)).T
    gap[...] = ce_ref[...] - ve
    squares = start * start
    sums = [jnp.sum(squares), jnp.sum(squares * gap[...])]
    for load in loads[3:]:
        load.wait()
    pl.semaphore_wait(barrier, R * C - 1)

    def reduce_start(i, values):
        rows = [jnp.broadcast_to(v.reshape(1, 1), (1, 128)) for v in values]
        rows += [jnp.zeros((1, 128), jnp.float32)] * (8 - len(rows))
        sa[i, c] = jnp.concatenate(rows, axis=0)
        for d in range(1, C):
            send(sa.at[i, c], sa.at[i, c], sa_s.at[i, d], sa_r.at[i, d], (r, (c + d) % C))

    def reduce_middle(i):
        for d in range(1, C):
            wait(sa.at[i, (c - d + C) % C], sa_s.at[i, d], sa_r.at[i, d])
        sb[i, r] = jnp.sum(sa[i], axis=0)
        for d in range(1, R):
            send(sb.at[i, r], sb.at[i, r], sb_s.at[i, d], sb_r.at[i, d], ((r + d) % R, c))

    others = range(1, R * C)

    def place(d):
        at = (r * C + c + d) % (R * C)
        return at // C, at % C

    def whole_start(values):
        rows = [jnp.broadcast_to(v.reshape(1, 1), (1, 128)) for v in values]
        rows += [jnp.zeros((1, 128), jnp.float32)] * (8 - len(rows))
        sc[r * C + c] = jnp.concatenate(rows, axis=0)
        for d in others:
            send(sc.at[r * C + c], sc.at[r * C + c], sc_s.at[d], sc_r.at[d], place(d))

    def whole_end():
        for d in others:
            wait(sc.at[(r * C + c + R * C - d) % (R * C)], sc_s.at[d], sc_r.at[d])
        total = jnp.sum(sc[...], axis=0)
        return [total[j : j + 1, 0:1] for j in range(3)]

    def reduce_end(i):
        for d in range(1, R):
            wait(sb.at[i, (r - d + R) % R], sb_s.at[i, d], sb_r.at[i, d])
        total = jnp.sum(sb[i], axis=0)
        return [total[j : j + 1, 0:1] for j in range(3)]

    piece = lambda j: pl.ds(j * pp, pp)
    rows_of = lambda i: pl.ds(i * m, m)

    side = z // (NZ // 2)
    mirror = z + side * (NZ - 1 - 2 * z)

    def origin(n):
        o = n + (n + NZ - mirror) // NZ
        return o + side * (NZ - 1 - 2 * o)

    def zown(src, dst, ss, rs):
        for up in range(2):
            to = z + 2 * up - 1
            send(src, dst, ss.at[z, up], rs.at[z], (r, to * 2 + h), (to >= 0) & (to < NZ))

    def znext(o, slot, ss, rs):
        wait(slot, ss.at[o, 0], rs.at[o])
        up = (z - o - 1 + NZ) // NZ
        to = z + 2 * up - 1
        send(slot, slot, ss.at[o, 0], rs.at[o], (r, to * 2 + h), (to >= 0) & (to < NZ))

    def own_x(j):
        send(pv_ref.at[piece(j)], pvl.at[c, piece(j)], vx_s.at[j, z], vx_r.at[j, z], xpeer)

    def own_z(j):
        zown(pv_ref.at[piece(j)], pvl.at[c, piece(j)], vz_s.at[j, h], vz_r.at[j, h])

    zown(x_ref, ql.at[c], qz_s, qz_r)
    send(x_ref, ql.at[c], qx_s.at[z], qx_r.at[z], xpeer)
    for d in range(1, NY):
        send(pc_ref, pcl.at[r], cy_s.at[d], cy_r.at[d], ydev(d))
    send(pc_ref, pcl.at[r], cc_s.at[0], cc_r.at[0], kpeer)
    own_x(0)
    reduce_start(0, sums)

    def put_x(dst, t, rows, b, value):
        hi, lo = halves(value)
        dst[0, rows, b * ncl : (b + 1) * ncl] = hi
        dst[1, rows, b * ncl : (b + 1) * ncl] = lo

    def put_pc(b, value):
        hi, lo = halves(value)
        pc3[0, b] = hi
        pc3[1, b] = lo

    def put_pv(j, zz, hh, value):
        hi, lo = halves(value.T)
        for u in range(per):
            pvt[0, hh * per + u, zz, :, piece(j)] = hi[u * m : (u + 1) * m]
            pvt[1, hh * per + u, zz, :, piece(j)] = lo[u * m : (u + 1) * m]

    def first_rows(n):
        o = origin(n)
        slot = ql.at[o * 2 + h]
        znext(o, slot, qz_s, qz_r)
        send(slot, slot, qx_s.at[o], qx_r.at[o], xpeer)

    def shared_piece(n):
        o = origin(n)
        for hh in range(2):
            slot = pvl.at[o * 2 + hh, piece(0)]
            znext(o, slot, vz_s.at[0, hh], vz_r.at[0, hh])
            put_pv(0, o, hh, pvl[o * 2 + hh, piece(0), :])

    ql[c] = start
    put_pc(r, pc_ref[...])
    put_pv(0, z, h, pv_ref[piece(0), :])
    def image_of(ref, rows):
        total = None
        for b in range(R):
            cols = slice(b * npc, (b + 1) * npc)
            part = dot3((ref[0, rows, cols], ref[1, rows, cols]), (pc3[0, b], pc3[1, b]), NT)
            total = part if total is None else total + part
        return total

    def arrive(j, n):
        o = origin(n)
        slot = pvl.at[o * 2 + h, piece(j)]
        znext(o, slot, vz_s.at[j, h], vz_r.at[j, h])
        send(slot, slot, vx_s.at[j, o], vx_r.at[j, o], xpeer)
        put_pv(j, o, h, pvl[o * 2 + h, piece(j), :])

    def across(j, o):
        b = o * 2 + 1 - h
        wait(pvl.at[b, piece(j)], vx_s.at[j, o], vx_r.at[j, o])
        put_pv(j, o, 1 - h, pvl[b, piece(j), :])

    def points(j, scale):
        parts = [pvt[t, :, :, :, piece(j)].reshape(CHUNKS * R * m, pp) for t in range(2)]
        part = dot3((it[0], it[1]), parts, NN)
        acc1[:, piece(j)] = part
        wt[0, :, piece(j)], wt[1, :, piece(j)] = halves(part * scale * wtr[:, piece(j)])

    def flip(i, value):
        it[0, :, i * R * m : (i + 1) * R * m], it[1, :, i * R * m : (i + 1) * R * m] = halves(value.T)

    def first_image():
        for d in range(1, NY):
            slot = il1.at[yfrom(d) * 2 + k]
            wait(slot, jy_s.at[d], jy_r.at[d])
            send(slot, slot, jc_s.at[d], jc_r.at[d], kpeer)

    def flip_image():
        for d in range(NY):
            wait(il1.at[yfrom(d) * 2 + 1 - k], jc_s.at[d], jc_r.at[d])
        for i in range(CHUNKS):
            flip(i, jnp.concatenate([il1[b, rows_of(i), :] for b in range(R)], axis=0))

    def conduction():
        reduce_middle(0)
        wait(pcl.at[y * 2 + 1 - k], cc_s.at[0], cc_r.at[0])
        put_pc(y * 2 + 1 - k, pcl[y * 2 + 1 - k])
        for d in range(1, NY):
            slot = pcl.at[yfrom(d) * 2 + k]
            wait(slot, cy_s.at[d], cy_r.at[d])
            send(slot, slot, cc_s.at[d], cc_r.at[d], kpeer)
            put_pc(yfrom(d) * 2 + k, pcl[yfrom(d) * 2 + k])

    def send_image():
        for o in range(NZ):
            wait(ql.at[o * 2 + 1 - h], qx_s.at[o], qx_r.at[o])
        for b in range(C):
            put_x(xs, 0, slice(None), b, ql[b])
        for d in range(1, NY):
            b = yfrom(d) * 2 + 1 - k
            wait(pcl.at[b], cc_s.at[d], cc_r.at[d])
            put_pc(b, pcl[b])
        il1[r] = image_of(xs, slice(None))
        for d in range(1, NY):
            send(il1.at[r], il1.at[r], jy_s.at[d], jy_r.at[d], ydev(d))
        send(il1.at[r], il1.at[r], jc_s.at[0], jc_r.at[0], kpeer)

    def peer_piece():
        slot = pvl.at[z * 2 + 1 - h, piece(0)]
        wait(slot, vx_s.at[0, z], vx_r.at[0, z])
        zown(slot, slot, vz_s.at[0, 1 - h], vz_r.at[0, 1 - h])

    def peer_put():
        put_pv(0, z, 1 - h, pvl[z * 2 + 1 - h, piece(0), :])

    def flip_weights():
        load_w.wait()
        wtr[...] = wv[...].T

    def own_piece(j):
        own_z(j)
        put_pv(j, z, h, pv_ref[piece(j), :])

    def crossed(j, n):
        across(j, z if n == 0 else origin(n - 1))

    first = {}

    def normalise():
        total, gaps, _ = reduce_end(0)
        mean = total / count
        first["mean"] = mean
        first["scale"] = 1.0 / jnp.sqrt(mean + EPS)
        first["shift"] = (gaps / count) / (mean + EPS)

    def finish_piece(j):
        if not first:
            normalise()
        points(j, first["scale"])

    opening = dict(
        u=lambda: own_z(0),
        f=first_rows, q=peer_piece, g=peer_put, o=own_x, w=own_piece, s=shared_piece, a=arrive, x=crossed,
        t=flip_weights, c=conduction, i=send_image, j=first_image, l=flip_image, p=finish_piece,
    )
    for name in OPENING:
        opening[name[0]](*(int(v) for v in name[1:]))
    mean, scale, shift = first["mean"], first["scale"], first["shift"]
    q1[...] = start * scale
    gap[...] = gap[...] - shift

    zero = jnp.zeros((m, ncl), jnp.float32)
    sums = {0: [zero, zero], 1: [zero, zero, zero]}
    state = {}
    counts = [0, 0, 0]

    group = lambda g: range(g * GROUP, (g + 1) * GROUP)

    def back(s, g):
        lhs = [pvt[t, g * GROUP : (g + 1) * GROUP].reshape(GROUP * R * m, np_) for t in range(2)]
        part = dot3(lhs, (wt[0], wt[1]), NT)
        for u, i in enumerate(group(g)):
            for b in range(R):
                at = (u * R + b) * m
                bk[s, i, b % 2, b // 2] = part[at : at + m]
            send(bk.at[s, i, 1 - k], cr.at[s, i], cr_s.at[s, i], cr_r.at[s, i], kpeer)

    def spread(s, i):
        wait(cr.at[s, i], cr_s.at[s, i], cr_r.at[s, i])
        for d in range(1, NY):
            yy = (y + d) % NY
            bk[s, i, k, yy] = bk[s, i, k, yy] + cr[s, i, yy]
            send(bk.at[s, i, k, yy], yr.at[s, i, d], yr_s.at[s, i, d], yr_r.at[s, i, d], ydev(d))

    def kernel_part(s, i):
        summed = bk[s, i, k, y] + cr[s, i, y]
        for d in range(1, NY):
            wait(yr.at[s, i, d], yr_s.at[s, i, d], yr_r.at[s, i, d])
            summed = summed + yr[s, i, d]
        flat = halves(summed)
        for b in range(R):
            part = dot3(flat, (pc3[0, b], pc3[1, b]), NN)
            for u in range(npc // ncl):
                at = b * (npc // ncl) + u
                kb[s, i, at % 2, at // 2] = part[:, u * ncl : (u + 1) * ncl]
        send(kb.at[s, i, 1 - h], xr.at[s, i], xr_s.at[s, i], xr_r.at[s, i], xpeer)

    def zsum(s, i):
        wait(xr.at[s, i], xr_s.at[s, i], xr_r.at[s, i])
        for d in far:
            zz = (z + d) % NZ
            kb[s, i, h, zz] = kb[s, i, h, zz] + xr[s, i, zz]
            send(kb.at[s, i, h, zz], zr.at[s, i, d], zr_s.at[s, i, d], zr_r.at[s, i, d], zdev(d))

    def vector_part(s, i):
        rows = rows_of(i)
        total = kb[s, i, h, z] + xr[s, i, z]
        for d in near:
            wait(zr.at[s, i, d], zr_s.at[s, i, d], zr_r.at[s, i, d])
            total = total + zr[s, i, d]
        before = q1[rows, :]
        if s == 0:
            image = gap[rows, :] * before - total
            hl[c, rows, :] = image
            own = hl.at[c, rows]
            for d in near:
                send(own, own, gz_s.at[i, d], gz_r.at[i, d], zdev(d))
            send(own, own, gx_s.at[i, 0], gx_r.at[i, 0], xpeer)
            sums[0][0] += before * image
            sums[0][1] += image * image
        else:
            vector = (hl[c, rows, :] - state["move"] * before) / state["beta"]
            image = gap[rows, :] * vector - total
            acc1[rows, :ncl] = vector
            acc1[rows, ncl : 2 * ncl] = image
            sums[1][0] += vector * image
            sums[1][1] += image * image
            sums[1][2] += before * image
        counts[s] += 1
        if counts[s] == CHUNKS:
            partial = [jnp.sum(v) for v in sums[s]]
            reduce_start(1, partial) if s == 0 else whole_start(partial)

    def forward(s, i):
        for d in near:
            slot = hl.at[zfrom(d) * 2 + h, rows_of(i)]
            wait(slot, gz_s.at[i, d], gz_r.at[i, d])
            send(slot, slot, gx_s.at[i, d], gx_r.at[i, d], xpeer)

    def image_part(s, i):
        rows = rows_of(i)
        for d in [0] + near:
            wait(hl.at[zfrom(d) * 2 + 1 - h, rows], gx_s.at[i, d], gx_r.at[i, d])
        for b in range(C):
            put_x(xh, 1, rows, b, hl[b, rows, :])
        il2[i, r] = image_of(xh, rows)
        own = il2.at[i, r]
        for d in range(1, NY):
            send(own, own, iy_s.at[i, d], iy_r.at[i, d], ydev(d))
        send(own, own, ic_s.at[i, 0], ic_r.at[i, 0], kpeer)

    def exchange(s, i):
        for d in range(1, NY):
            slot = il2.at[i, yfrom(d) * 2 + k]
            wait(slot, iy_s.at[i, d], iy_r.at[i, d])
            send(slot, slot, ic_s.at[i, d], ic_r.at[i, d], kpeer)

    def scalars(s, i):
        reduce_middle(1)

    def add_points(s, g):
        for i in group(g):
            for d in range(NY):
                wait(il2.at[i, yfrom(d) * 2 + 1 - k], ic_s.at[i, d], ic_r.at[i, d])
            flip(i, il2[i].reshape(R * m, pcn))
        cols = slice(g * GROUP * R * m, (g + 1) * GROUP * R * m)
        counts[2] += 1
        last = counts[2] == CHUNKS // GROUP
        if last:
            cross, square, _ = reduce_end(1)
            inside, norm = cross / count, mean / (mean + EPS)
            move = inside - shift * (EPS / (mean + EPS))
            beta = jnp.sqrt(square / count - 2.0 * move * inside + move * move * norm + EPS)
            state.update(move=move, beta=beta, norm=norm, alpha=shift + move)
            inverse, drop = 1.0 / beta, move * scale
        for j in range(PIECES):
            lanes = piece(j)
            rhs = [pvt[t, g * GROUP : (g + 1) * GROUP, :, :, lanes].reshape(GROUP * R * m, pp) for t in range(2)]
            part = dot3((it[0, :, cols], it[1, :, cols]), rhs, NN)
            if counts[2] > 1:
                part = acc2[:, lanes] + part
            if last:
                part = (part - drop * acc1[:, lanes]) * inverse * wtr[:, lanes]
                wt[0, :, lanes], wt[1, :, lanes] = halves(part)
            else:
                acc2[:, lanes] = part

    events = dict(
        b=back, s=spread, k=kernel_part, z=zsum, h=vector_part, f=forward,
        m=image_part, e=exchange, a=add_points, r=scalars,
    )
    for s, order in enumerate((FIRST, SECOND)):
        for name in order:
            events[name[0]](s, int(name[1:]))

    def settle(ops):
        for when, args in ops:
            finish = lambda: copy(*args).wait_send()
            pl.when(when)(finish) if when is not None else finish()

    settle(pending[: -len(others)])
    cross, square, older = [v / count for v in whole_end()]
    move, beta, norm, alpha = (state[n] for n in ("move", "beta", "norm", "alpha"))
    size = 1.0 - EPS / (beta * beta)
    overlap = (EPS / (mean + EPS)) * alpha / beta
    step = cross - shift * (EPS / (beta * beta))
    squared = (
        square + step * step * size + beta * beta * norm
        - 2.0 * step * cross - 2.0 * beta * older + 2.0 * step * beta * overlap
    )
    beta2 = jnp.sqrt(squared + EPS)
    vector, image = acc1[:nv, :ncl], acc1[:nv, ncl : 2 * ncl]
    out_ref[...] = (image - step * vector - beta * q1[...]) / beta2
    for j, value in enumerate((alpha, beta, shift + step, beta2)):
        coef_ref[j : j + 1, :] = jnp.broadcast_to(value, (1, 128))
    settle(pending[-len(others) :])


def hand_over(vector_ref, coef_ref, out_ref, out_coef_ref):
    out_ref[...] = vector_ref[...]
    for j in range(4):
        out_coef_ref[j] = coef_ref[j, 0]


def fused_shards(R, C, excitons, valence_energy, conduction_energy, psi_valence, psi_conduction, screened):
    nv, nc = excitons.shape
    pr, pcn = screened.shape
    nvl, npc = psi_valence.shape[1], psi_conduction.shape[1]
    f32, bf16 = jnp.float32, jnp.bfloat16
    NY, NZ = R // 2, C // 2
    n, m = CHUNKS, nv // CHUNKS
    vm, dma = pltpu.VMEM, pltpu.SemaphoreType.DMA
    count = float(NV * NC)
    scratch = [
        vm((C, nv, nc), f32), vm((C, nv, nc), f32), vm((C, pr, nvl), f32), vm((R, pcn, npc), f32),
        vm((R, nv, pcn), f32), vm((n, R, m, pcn), f32),
        vm((2, n, 2, NY, m, pcn), f32), vm((2, n, NY, m, pcn), f32), vm((2, n, NY, m, pcn), f32),
        vm((2, n, 2, NZ, m, nc), f32), vm((2, n, NZ, m, nc), f32), vm((2, n, NZ, m, nc), f32),
        vm((2, C, 8, 128), f32), vm((2, R, 8, 128), f32), vm((R * C, 8, 128), f32),
        vm((2, n, R, m, pr), bf16), vm((2, R, pcn, npc), bf16), vm((2, nv, NC), bf16), vm((2, nv, NC), bf16),
        vm((2, pcn, NV), bf16), vm((2, pcn, pr), bf16),
        vm((pcn, pr), f32), vm((pcn, pr), f32), vm((pcn, pr), f32), vm((pr, pcn), f32),
        vm((nv, nc), f32), vm((nv, nc), f32),
        vm((nv, nc), f32), vm((1, nv), f32), vm((1, nc), f32), vm((pr, nvl), f32), vm((pcn, npc), f32),
        dma(()), dma((5,)),
    ]
    pairs = [
        [(NZ, 2), (NZ,)], (NZ,), [(PIECES, 2, NZ, 2), (PIECES, 2, NZ)], (PIECES, NZ), (NY,), (NY,), (NY,), (NY,), (n, NY), (n, NY), (n, NZ), (n, NZ),
        (2, n), (2, n, NY), (2, n), (2, n, NZ), (2, C), (2, R), (R * C,),
    ]
    for shape in pairs:
        both = shape if isinstance(shape, list) else [shape, shape]
        scratch += [dma(v) for v in both]
    vector, coef = pl.pallas_call(
        lambda *refs: fused(R, C, count, *refs),
        out_shape=(jax.ShapeDtypeStruct((nv, nc), f32), jax.ShapeDtypeStruct((8, 128), f32)),
        in_specs=[pl.BlockSpec(memory_space=pl.ANY)] * 6,
        out_specs=(pl.BlockSpec(memory_space=vm), pl.BlockSpec(memory_space=vm)),
        scratch_shapes=scratch,
        compiler_params=pltpu.CompilerParams(collective_id=0, has_side_effects=True, vmem_limit_bytes=67043328),
    )(excitons, valence_energy.reshape(1, nv), conduction_energy.reshape(1, nc), psi_valence, psi_conduction, screened)
    return pl.pallas_call(
        hand_over,
        out_shape=(jax.ShapeDtypeStruct((nv, nc), f32), jax.ShapeDtypeStruct((4,), f32)),
        in_specs=[pl.BlockSpec(memory_space=vm)] * 2,
        out_specs=(pl.BlockSpec(memory_space=vm), pl.BlockSpec(memory_space=pltpu.SMEM)),
    )(vector, coef)


def solution(mesh):
    R, C = mesh.shape["row"], mesh.shape["col"]
    covered = max(int(v[1:]) for v in OPENING if v[0] == "f") == C // 2 - 2
    aligned = covered and C == 2 * R and R % 2 == 0 and STEPS == 2 and NV == NC and (NV // R) % (16 * CHUNKS) == 0 and (NV // R) % 128 == 0 and (NC // C) % 128 == 0
    body = (lambda *args: fused_shards(R, C, *args)) if aligned else shards
    return jax.shard_map(
        body,
        mesh=mesh,
        in_specs=(
            P("row", "col"),
            P("row"),
            P("col"),
            P("row", "col"),
            P("col", "row"),
            P("row", "col"),
        ),
        out_specs=(P("row", "col"), P()),
        check_vma=False,
    )
```

```python
import jax
import jax.numpy as jnp
from jax import lax
from jax.experimental import pallas as pl
from jax.experimental.pallas import tpu as pltpu
from jax.sharding import PartitionSpec as P

NV = 1024
NC = 1024
STEPS = 2


EPS = 1e-06


def shards(excitons, valence_energy, conduction_energy, psi_valence, psi_conduction, screened):
    high = lax.Precision.HIGHEST
    count = NV * NC
    energy_gap = conduction_energy[None, :] - valence_energy[:, None]
    total = lax.psum(jnp.sum(excitons * excitons), ("row", "col"))
    vector = excitons / jnp.sqrt(total / count + EPS)
    previous = jnp.zeros_like(vector)
    beta_prev = jnp.zeros((), jnp.float32)
    values = []
    for step in range(STEPS):
        panel_valence = lax.all_gather(psi_valence, "col", axis=1, tiled=True)
        panel_conduction = lax.all_gather(psi_conduction, "row", axis=1, tiled=True)
        full_rows = lax.all_gather(vector, "col", axis=1, tiled=True)
        image_block = jnp.dot(full_rows, panel_conduction.T, precision=high)
        image_columns = lax.all_gather(image_block, "row", axis=0, tiled=True)
        points = jnp.dot(panel_valence, image_columns, precision=high)
        weighted = points * screened
        back_valence = lax.psum_scatter(
            jnp.dot(panel_valence.T, weighted, precision=high),
            "row",
            scatter_dimension=0,
            tiled=True,
        )
        back_flipped = back_valence.T
        kernel_flipped = lax.psum_scatter(
            jnp.dot(panel_conduction.T, back_flipped, precision=high),
            "col",
            scatter_dimension=0,
            tiled=True,
        )
        image = energy_gap * vector - kernel_flipped.T
        cross, square, older = lax.psum(
            (jnp.sum(vector * image), jnp.sum(image * image), jnp.sum(previous * image)),
            ("row", "col"),
        )
        alpha = cross / count
        residual = image - alpha * vector - beta_prev * previous
        squared = (
            square / count - alpha * alpha - 2.0 * beta_prev * older / count + beta_prev * beta_prev
        )
        beta = jnp.sqrt(squared + EPS)
        previous = vector
        vector = residual / beta
        beta_prev = beta
        values.append(alpha)
        values.append(beta)
    return (vector, jnp.stack(values))


MESH = pl.DeviceIdType.MESH
NN = (((1,), (0,)), ((), ()))
NT = (((1,), (1,)), ((), ()))
CHUNKS = 8
GROUP = 2
PIECES = 4
OPENING = (
    "o2", "t", "o3", "w3", "f0", "w2", "w1", "f1", "f2", "a10", "a21", "a20", "a12", "u",
    "o1", "c", "a22", "i", "x20", "x22", "a11", "q", "a30", "s1", "j", "x23", "x21", "s0",
    "a31", "g", "x11", "l", "x10", "x12", "a32", "x13", "x30", "p1", "p2", "x31", "s2", "x32",
    "p0", "x33", "p3",
)
FIRST = (
    "b0", "b1", "s0", "s2", "b3", "s1", "b2", "k0", "s6", "s5", "k2", "s4", "s7", "s3",
    "k1", "z0", "z2", "k6", "z1", "k4", "h0", "h2", "k3", "k5", "z4", "h1", "z3", "z5",
    "z6", "k7", "f0", "f1", "h4", "h3", "f2", "z7", "h5", "m0", "h6", "f4", "m2", "f3",
    "m1", "h7", "f5", "m4", "e2", "e0", "f6", "m3", "f7", "m5", "m6", "r0", "e3", "e4",
    "m7", "e1", "a1", "e6", "e5", "a0", "e7", "a2", "a3",
)
SECOND = (
    "b0", "b1", "s0", "b3", "s3", "b2", "s2", "k0", "s7", "s6", "k3", "k2", "s1", "s4",
    "s5", "z0", "k7", "z3", "k6", "z2", "k1", "z7", "k4", "z6", "k5", "z1", "z4", "z5",
    "h6", "h1", "h0", "h3", "h4", "h2", "h7", "h5",
)


def halves(value):
    hi = value.astype(jnp.bfloat16)
    return hi, (value - hi.astype(jnp.float32)).astype(jnp.bfloat16)


def dot3(a, b, dims):
    dot = lambda u, v: lax.dot_general(u, v, dims, preferred_element_type=jnp.float32)
    return dot(a[0], b[0]) + (dot(a[0], b[1]) + dot(a[1], b[0]))


def fused(
    R, C, count,
    x_in, ve_in, ce_in, pv_in, pc_in, w_ref,
    out_ref, coef_ref,
    ql, hl, pvl, pcl, il1, il2, bk, cr, yr, kb, xr, zr, sa, sb, sc,
    pvt, pc3, xs, xh, it, wt, acc1, acc2, wtr, wv, q1, gap,
    x_ref, ve_ref, ce_ref, pv_ref, pc_ref, w_s, in_s, qz_s, qz_r, qx_s, qx_r, vz_s, vz_r, vx_s, vx_r, cy_s, cy_r, cc_s, cc_r,
    jy_s, jy_r, jc_s, jc_r, iy_s, iy_r, ic_s, ic_r, gz_s, gz_r, gx_s, gx_r,
    cr_s, cr_r, yr_s, yr_r, xr_s, xr_r, zr_s, zr_r, sa_s, sa_r, sb_s, sb_r, sc_s, sc_r,
):
    NY, NZ = R // 2, C // 2
    r, c = lax.axis_index("row"), lax.axis_index("col")
    y, k, z, h = r // 2, r % 2, c // 2, c % 2
    nv, ncl = x_ref.shape
    np_, nvl = pv_ref.shape
    pcn, npc = pc_ref.shape
    m = nv // CHUNKS
    per = CHUNKS // 2
    pp = np_ // PIECES
    pending = []

    def copy(src, dst, ss, rs, dev):
        return pltpu.make_async_remote_copy(
            src_ref=src, dst_ref=dst, send_sem=ss, recv_sem=rs, device_id=dev, device_id_type=MESH
        )

    def send(src, dst, ss, rs, dev, when=None):
        args = (src, dst, ss, rs, dev)
        start = lambda: copy(*args).start()
        pl.when(when)(start) if when is not None else start()
        pending.append((when, args))

    def wait(dst, ss, rs):
        copy(dst, dst, ss, rs, (r, c)).wait_recv()

    zdev = lambda d: (r, ((z + d) % NZ) * 2 + h)
    zfrom = lambda d: (z - d + NZ) % NZ
    xpeer = (r, z * 2 + 1 - h)
    ydev = lambda d: (((y + d) % NY) * 2 + k, c)
    yfrom = lambda d: (y - d + NY) % NY
    kpeer = (y * 2 + 1 - k, c)
    near = [d for d in range(1, NZ) if d in (1, NZ - 1)] + [d for d in range(2, NZ - 1)]
    far = near[2:] + near[:2]

    loads = [
        pltpu.make_async_copy(src, dst, in_s.at[j])
        for j, (src, dst) in enumerate(
            ((x_in, x_ref), (ve_in, ve_ref), (ce_in, ce_ref), (pv_in, pv_ref), (pc_in, pc_ref))
        )
    ]
    load_w = pltpu.make_async_copy(w_ref, wv, w_s)
    for load in loads + [load_w]:
        load.start()
    barrier = pltpu.get_barrier_semaphore()
    for d in range(1, R * C):
        at = (r * C + c + d) % (R * C)
        pl.semaphore_signal(barrier, inc=1, device_id=(at // C, at % C), device_id_type=MESH)

    for load in loads[:3]:
        load.wait()
    start = x_ref[...]
    ve = jnp.broadcast_to(ve_ref[...], (ncl, nv)).T
    gap[...] = ce_ref[...] - ve
    squares = start * start
    sums = [jnp.sum(squares), jnp.sum(squares * gap[...])]
    for load in loads[3:]:
        load.wait()
    pl.semaphore_wait(barrier, R * C - 1)

    def reduce_start(i, values):
        rows = [jnp.broadcast_to(v.reshape(1, 1), (1, 128)) for v in values]
        rows += [jnp.zeros((1, 128), jnp.float32)] * (8 - len(rows))
        sa[i, c] = jnp.concatenate(rows, axis=0)
        for d in range(1, C):
            send(sa.at[i, c], sa.at[i, c], sa_s.at[i, d], sa_r.at[i, d], (r, (c + d) % C))

    def reduce_middle(i):
        for d in range(1, C):
            wait(sa.at[i, (c - d + C) % C], sa_s.at[i, d], sa_r.at[i, d])
        sb[i, r] = jnp.sum(sa[i], axis=0)
        for d in range(1, R):
            send(sb.at[i, r], sb.at[i, r], sb_s.at[i, d], sb_r.at[i, d], ((r + d) % R, c))

    others = range(1, R * C)

    def place(d):
        at = (r * C + c + d) % (R * C)
        return at // C, at % C

    def whole_start(values):
        rows = [jnp.broadcast_to(v.reshape(1, 1), (1, 128)) for v in values]
        rows += [jnp.zeros((1, 128), jnp.float32)] * (8 - len(rows))
        sc[r * C + c] = jnp.concatenate(rows, axis=0)
        for d in others:
            send(sc.at[r * C + c], sc.at[r * C + c], sc_s.at[d], sc_r.at[d], place(d))

    def whole_end():
        for d in others:
            wait(sc.at[(r * C + c + R * C - d) % (R * C)], sc_s.at[d], sc_r.at[d])
        total = jnp.sum(sc[...], axis=0)
        return [total[j : j + 1, 0:1] for j in range(3)]

    def reduce_end(i):
        for d in range(1, R):
            wait(sb.at[i, (r - d + R) % R], sb_s.at[i, d], sb_r.at[i, d])
        total = jnp.sum(sb[i], axis=0)
        return [total[j : j + 1, 0:1] for j in range(3)]

    piece = lambda j: pl.ds(j * pp, pp)
    rows_of = lambda i: pl.ds(i * m, m)

    side = z // (NZ // 2)
    mirror = z + side * (NZ - 1 - 2 * z)

    def origin(n):
        o = n + (n + NZ - mirror) // NZ
        return o + side * (NZ - 1 - 2 * o)

    def zown(src, dst, ss, rs):
        for up in range(2):
            to = z + 2 * up - 1
            send(src, dst, ss.at[z, up], rs.at[z], (r, to * 2 + h), (to >= 0) & (to < NZ))

    def znext(o, slot, ss, rs):
        wait(slot, ss.at[o, 0], rs.at[o])
        up = (z - o - 1 + NZ) // NZ
        to = z + 2 * up - 1
        send(slot, slot, ss.at[o, 0], rs.at[o], (r, to * 2 + h), (to >= 0) & (to < NZ))

    def own_x(j):
        send(pv_ref.at[piece(j)], pvl.at[c, piece(j)], vx_s.at[j, z], vx_r.at[j, z], xpeer)

    def own_z(j):
        zown(pv_ref.at[piece(j)], pvl.at[c, piece(j)], vz_s.at[j, h], vz_r.at[j, h])

    zown(x_ref, ql.at[c], qz_s, qz_r)
    send(x_ref, ql.at[c], qx_s.at[z], qx_r.at[z], xpeer)
    for d in range(1, NY):
        send(pc_ref, pcl.at[r], cy_s.at[d], cy_r.at[d], ydev(d))
    send(pc_ref, pcl.at[r], cc_s.at[0], cc_r.at[0], kpeer)
    own_x(0)
    reduce_start(0, sums)

    def put_x(dst, t, rows, b, value):
        hi, lo = halves(value)
        dst[0, rows, b * ncl : (b + 1) * ncl] = hi
        dst[1, rows, b * ncl : (b + 1) * ncl] = lo

    def put_pc(b, value):
        hi, lo = halves(value)
        pc3[0, b] = hi
        pc3[1, b] = lo

    def put_pv(j, zz, hh, value):
        hi, lo = halves(value.T)
        for u in range(per):
            pvt[0, hh * per + u, zz, :, piece(j)] = hi[u * m : (u + 1) * m]
            pvt[1, hh * per + u, zz, :, piece(j)] = lo[u * m : (u + 1) * m]

    def first_rows(n):
        o = origin(n)
        slot = ql.at[o * 2 + h]
        znext(o, slot, qz_s, qz_r)
        send(slot, slot, qx_s.at[o], qx_r.at[o], xpeer)

    def shared_piece(n):
        o = origin(n)
        for hh in range(2):
            slot = pvl.at[o * 2 + hh, piece(0)]
            znext(o, slot, vz_s.at[0, hh], vz_r.at[0, hh])
            put_pv(0, o, hh, pvl[o * 2 + hh, piece(0), :])

    ql[c] = start
    put_pc(r, pc_ref[...])
    put_pv(0, z, h, pv_ref[piece(0), :])
    def image_of(ref, rows):
        total = None
        for b in range(R):
            cols = slice(b * npc, (b + 1) * npc)
            part = dot3((ref[0, rows, cols], ref[1, rows, cols]), (pc3[0, b], pc3[1, b]), NT)
            total = part if total is None else total + part
        return total

    def arrive(j, n):
        o = origin(n)
        slot = pvl.at[o * 2 + h, piece(j)]
        znext(o, slot, vz_s.at[j, h], vz_r.at[j, h])
        send(slot, slot, vx_s.at[j, o], vx_r.at[j, o], xpeer)
        put_pv(j, o, h, pvl[o * 2 + h, piece(j), :])

    def across(j, o):
        b = o * 2 + 1 - h
        wait(pvl.at[b, piece(j)], vx_s.at[j, o], vx_r.at[j, o])
        put_pv(j, o, 1 - h, pvl[b, piece(j), :])

    def points(j, scale):
        parts = [pvt[t, :, :, :, piece(j)].reshape(CHUNKS * R * m, pp) for t in range(2)]
        part = dot3((it[0], it[1]), parts, NN)
        acc1[:, piece(j)] = part
        wt[0, :, piece(j)], wt[1, :, piece(j)] = halves(part * scale * wtr[:, piece(j)])

    def flip(i, value):
        it[0, :, i * R * m : (i + 1) * R * m], it[1, :, i * R * m : (i + 1) * R * m] = halves(value.T)

    def first_image():
        for d in range(1, NY):
            slot = il1.at[yfrom(d) * 2 + k]
            wait(slot, jy_s.at[d], jy_r.at[d])
            send(slot, slot, jc_s.at[d], jc_r.at[d], kpeer)

    def flip_image():
        for d in range(NY):
            wait(il1.at[yfrom(d) * 2 + 1 - k], jc_s.at[d], jc_r.at[d])
        for i in range(CHUNKS):
            flip(i, jnp.concatenate([il1[b, rows_of(i), :] for b in range(R)], axis=0))

    def conduction():
        reduce_middle(0)
        wait(pcl.at[y * 2 + 1 - k], cc_s.at[0], cc_r.at[0])
        put_pc(y * 2 + 1 - k, pcl[y * 2 + 1 - k])
        for d in range(1, NY):
            slot = pcl.at[yfrom(d) * 2 + k]
            wait(slot, cy_s.at[d], cy_r.at[d])
            send(slot, slot, cc_s.at[d], cc_r.at[d], kpeer)
            put_pc(yfrom(d) * 2 + k, pcl[yfrom(d) * 2 + k])

    def send_image():
        for o in range(NZ):
            wait(ql.at[o * 2 + 1 - h], qx_s.at[o], qx_r.at[o])
        for b in range(C):
            put_x(xs, 0, slice(None), b, ql[b])
        for d in range(1, NY):
            b = yfrom(d) * 2 + 1 - k
            wait(pcl.at[b], cc_s.at[d], cc_r.at[d])
            put_pc(b, pcl[b])
        il1[r] = image_of(xs, slice(None))
        for d in range(1, NY):
            send(il1.at[r], il1.at[r], jy_s.at[d], jy_r.at[d], ydev(d))
        send(il1.at[r], il1.at[r], jc_s.at[0], jc_r.at[0], kpeer)

    def peer_piece():
        slot = pvl.at[z * 2 + 1 - h, piece(0)]
        wait(slot, vx_s.at[0, z], vx_r.at[0, z])
        zown(slot, slot, vz_s.at[0, 1 - h], vz_r.at[0, 1 - h])

    def peer_put():
        put_pv(0, z, 1 - h, pvl[z * 2 + 1 - h, piece(0), :])

    def flip_weights():
        load_w.wait()
        wtr[...] = wv[...].T

    def own_piece(j):
        own_z(j)
        put_pv(j, z, h, pv_ref[piece(j), :])

    def crossed(j, n):
        across(j, z if n == 0 else origin(n - 1))

    first = {}

    def normalise():
        total, gaps, _ = reduce_end(0)
        mean = total / count
        first["mean"] = mean
        first["scale"] = 1.0 / jnp.sqrt(mean + EPS)
        first["shift"] = (gaps / count) / (mean + EPS)

    def finish_piece(j):
        if not first:
            normalise()
        points(j, first["scale"])

    opening = dict(
        u=lambda: own_z(0),
        f=first_rows, q=peer_piece, g=peer_put, o=own_x, w=own_piece, s=shared_piece, a=arrive, x=crossed,
        t=flip_weights, c=conduction, i=send_image, j=first_image, l=flip_image, p=finish_piece,
    )
    for name in OPENING:
        opening[name[0]](*(int(v) for v in name[1:]))
    mean, scale, shift = first["mean"], first["scale"], first["shift"]
    q1[...] = start * scale
    gap[...] = gap[...] - shift

    zero = jnp.zeros((m, ncl), jnp.float32)
    sums = {0: [zero, zero], 1: [zero, zero, zero]}
    state = {}
    counts = [0, 0, 0]

    group = lambda g: range(g * GROUP, (g + 1) * GROUP)

    def back(s, g):
        lhs = [pvt[t, g * GROUP : (g + 1) * GROUP].reshape(GROUP * R * m, np_) for t in range(2)]
        part = dot3(lhs, (wt[0], wt[1]), NT)
        for u, i in enumerate(group(g)):
            for b in range(R):
                at = (u * R + b) * m
                bk[s, i, b % 2, b // 2] = part[at : at + m]
            send(bk.at[s, i, 1 - k], cr.at[s, i], cr_s.at[s, i], cr_r.at[s, i], kpeer)

    def spread(s, i):
        wait(cr.at[s, i], cr_s.at[s, i], cr_r.at[s, i])
        for d in range(1, NY):
            yy = (y + d) % NY
            bk[s, i, k, yy] = bk[s, i, k, yy] + cr[s, i, yy]
            send(bk.at[s, i, k, yy], yr.at[s, i, d], yr_s.at[s, i, d], yr_r.at[s, i, d], ydev(d))

    def kernel_part(s, i):
        summed = bk[s, i, k, y] + cr[s, i, y]
        for d in range(1, NY):
            wait(yr.at[s, i, d], yr_s.at[s, i, d], yr_r.at[s, i, d])
            summed = summed + yr[s, i, d]
        flat = halves(summed)
        for b in range(R):
            part = dot3(flat, (pc3[0, b], pc3[1, b]), NN)
            for u in range(npc // ncl):
                at = b * (npc // ncl) + u
                kb[s, i, at % 2, at // 2] = part[:, u * ncl : (u + 1) * ncl]
        send(kb.at[s, i, 1 - h], xr.at[s, i], xr_s.at[s, i], xr_r.at[s, i], xpeer)

    def zsum(s, i):
        wait(xr.at[s, i], xr_s.at[s, i], xr_r.at[s, i])
        for d in far:
            zz = (z + d) % NZ
            kb[s, i, h, zz] = kb[s, i, h, zz] + xr[s, i, zz]
            send(kb.at[s, i, h, zz], zr.at[s, i, d], zr_s.at[s, i, d], zr_r.at[s, i, d], zdev(d))

    def vector_part(s, i):
        rows = rows_of(i)
        total = kb[s, i, h, z] + xr[s, i, z]
        for d in near:
            wait(zr.at[s, i, d], zr_s.at[s, i, d], zr_r.at[s, i, d])
            total = total + zr[s, i, d]
        before = q1[rows, :]
        if s == 0:
            image = gap[rows, :] * before - total
            hl[c, rows, :] = image
            own = hl.at[c, rows]
            for d in near:
                send(own, own, gz_s.at[i, d], gz_r.at[i, d], zdev(d))
            send(own, own, gx_s.at[i, 0], gx_r.at[i, 0], xpeer)
            sums[0][0] += before * image
            sums[0][1] += image * image
        else:
            vector = (hl[c, rows, :] - state["move"] * before) / state["beta"]
            image = gap[rows, :] * vector - total
            acc1[rows, :ncl] = vector
            acc1[rows, ncl : 2 * ncl] = image
            sums[1][0] += vector * image
            sums[1][1] += image * image
            sums[1][2] += before * image
        counts[s] += 1
        if counts[s] == CHUNKS:
            partial = [jnp.sum(v) for v in sums[s]]
            reduce_start(1, partial) if s == 0 else whole_start(partial)

    def forward(s, i):
        for d in near:
            slot = hl.at[zfrom(d) * 2 + h, rows_of(i)]
            wait(slot, gz_s.at[i, d], gz_r.at[i, d])
            send(slot, slot, gx_s.at[i, d], gx_r.at[i, d], xpeer)

    def image_part(s, i):
        rows = rows_of(i)
        for d in [0] + near:
            wait(hl.at[zfrom(d) * 2 + 1 - h, rows], gx_s.at[i, d], gx_r.at[i, d])
        for b in range(C):
            put_x(xh, 1, rows, b, hl[b, rows, :])
        il2[i, r] = image_of(xh, rows)
        own = il2.at[i, r]
        for d in range(1, NY):
            send(own, own, iy_s.at[i, d], iy_r.at[i, d], ydev(d))
        send(own, own, ic_s.at[i, 0], ic_r.at[i, 0], kpeer)

    def exchange(s, i):
        for d in range(1, NY):
            slot = il2.at[i, yfrom(d) * 2 + k]
            wait(slot, iy_s.at[i, d], iy_r.at[i, d])
            send(slot, slot, ic_s.at[i, d], ic_r.at[i, d], kpeer)

    def scalars(s, i):
        reduce_middle(1)

    def add_points(s, g):
        for i in group(g):
            for d in range(NY):
                wait(il2.at[i, yfrom(d) * 2 + 1 - k], ic_s.at[i, d], ic_r.at[i, d])
            flip(i, il2[i].reshape(R * m, pcn))
        cols = slice(g * GROUP * R * m, (g + 1) * GROUP * R * m)
        counts[2] += 1
        last = counts[2] == CHUNKS // GROUP
        if last:
            cross, square, _ = reduce_end(1)
            inside, norm = cross / count, mean / (mean + EPS)
            move = inside - shift * (EPS / (mean + EPS))
            beta = jnp.sqrt(square / count - 2.0 * move * inside + move * move * norm + EPS)
            state.update(move=move, beta=beta, norm=norm, alpha=shift + move)
            inverse, drop = 1.0 / beta, move * scale
        for j in range(PIECES):
            lanes = piece(j)
            rhs = [pvt[t, g * GROUP : (g + 1) * GROUP, :, :, lanes].reshape(GROUP * R * m, pp) for t in range(2)]
            part = dot3((it[0, :, cols], it[1, :, cols]), rhs, NN)
            if counts[2] > 1:
                part = acc2[:, lanes] + part
            if last:
                part = (part - drop * acc1[:, lanes]) * inverse * wtr[:, lanes]
                wt[0, :, lanes], wt[1, :, lanes] = halves(part)
            else:
                acc2[:, lanes] = part

    events = dict(
        b=back, s=spread, k=kernel_part, z=zsum, h=vector_part, f=forward,
        m=image_part, e=exchange, a=add_points, r=scalars,
    )
    for s, order in enumerate((FIRST, SECOND)):
        for name in order:
            events[name[0]](s, int(name[1:]))

    def settle(ops):
        for when, args in ops:
            finish = lambda: copy(*args).wait_send()
            pl.when(when)(finish) if when is not None else finish()

    settle(pending[: -len(others)])
    cross, square, older = [v / count for v in whole_end()]
    move, beta, norm, alpha = (state[n] for n in ("move", "beta", "norm", "alpha"))
    size = 1.0 - EPS / (beta * beta)
    overlap = (EPS / (mean + EPS)) * alpha / beta
    step = cross - shift * (EPS / (beta * beta))
    squared = (
        square + step * step * size + beta * beta * norm
        - 2.0 * step * cross - 2.0 * beta * older + 2.0 * step * beta * overlap
    )
    beta2 = jnp.sqrt(squared + EPS)
    vector, image = acc1[:nv, :ncl], acc1[:nv, ncl : 2 * ncl]
    out_ref[...] = (image - step * vector - beta * q1[...]) / beta2
    for j, value in enumerate((alpha, beta, shift + step, beta2)):
        coef_ref[j : j + 1, :] = jnp.broadcast_to(value, (1, 128))
    settle(pending[-len(others) :])


def hand_over(vector_ref, coef_ref, out_ref, out_coef_ref):
    out_ref[...] = vector_ref[...]
    for j in range(4):
        out_coef_ref[j] = coef_ref[j, 0]


def fused_shards(R, C, excitons, valence_energy, conduction_energy, psi_valence, psi_conduction, screened):
    nv, nc = excitons.shape
    pr, pcn = screened.shape
    nvl, npc = psi_valence.shape[1], psi_conduction.shape[1]
    f32, bf16 = jnp.float32, jnp.bfloat16
    NY, NZ = R // 2, C // 2
    n, m = CHUNKS, nv // CHUNKS
    vm, dma = pltpu.VMEM, pltpu.SemaphoreType.DMA
    count = float(NV * NC)
    scratch = [
        vm((C, nv, nc), f32), vm((C, nv, nc), f32), vm((C, pr, nvl), f32), vm((R, pcn, npc), f32),
        vm((R, nv, pcn), f32), vm((n, R, m, pcn), f32),
        vm((2, n, 2, NY, m, pcn), f32), vm((2, n, NY, m, pcn), f32), vm((2, n, NY, m, pcn), f32),
        vm((2, n, 2, NZ, m, nc), f32), vm((2, n, NZ, m, nc), f32), vm((2, n, NZ, m, nc), f32),
        vm((2, C, 8, 128), f32), vm((2, R, 8, 128), f32), vm((R * C, 8, 128), f32),
        vm((2, n, R, m, pr), bf16), vm((2, R, pcn, npc), bf16), vm((2, nv, NC), bf16), vm((2, nv, NC), bf16),
        vm((2, pcn, NV), bf16), vm((2, pcn, pr), bf16),
        vm((pcn, pr), f32), vm((pcn, pr), f32), vm((pcn, pr), f32), vm((pr, pcn), f32),
        vm((nv, nc), f32), vm((nv, nc), f32),
        vm((nv, nc), f32), vm((1, nv), f32), vm((1, nc), f32), vm((pr, nvl), f32), vm((pcn, npc), f32),
        dma(()), dma((5,)),
    ]
    pairs = [
        [(NZ, 2), (NZ,)], (NZ,), [(PIECES, 2, NZ, 2), (PIECES, 2, NZ)], (PIECES, NZ), (NY,), (NY,), (NY,), (NY,), (n, NY), (n, NY), (n, NZ), (n, NZ),
        (2, n), (2, n, NY), (2, n), (2, n, NZ), (2, C), (2, R), (R * C,),
    ]
    for shape in pairs:
        both = shape if isinstance(shape, list) else [shape, shape]
        scratch += [dma(v) for v in both]
    vector, coef = pl.pallas_call(
        lambda *refs: fused(R, C, count, *refs),
        out_shape=(jax.ShapeDtypeStruct((nv, nc), f32), jax.ShapeDtypeStruct((8, 128), f32)),
        in_specs=[pl.BlockSpec(memory_space=pl.ANY)] * 6,
        out_specs=(pl.BlockSpec(memory_space=vm), pl.BlockSpec(memory_space=vm)),
        scratch_shapes=scratch,
        compiler_params=pltpu.CompilerParams(collective_id=0, has_side_effects=True, vmem_limit_bytes=67043328),
    )(excitons, valence_energy.reshape(1, nv), conduction_energy.reshape(1, nc), psi_valence, psi_conduction, screened)
    return pl.pallas_call(
        hand_over,
        out_shape=(jax.ShapeDtypeStruct((nv, nc), f32), jax.ShapeDtypeStruct((4,), f32)),
        in_specs=[pl.BlockSpec(memory_space=vm)] * 2,
        out_specs=(pl.BlockSpec(memory_space=vm), pl.BlockSpec(memory_space=pltpu.SMEM)),
    )(vector, coef)


def solution(mesh):
    R, C = mesh.shape["row"], mesh.shape["col"]
    covered = max(int(v[1:]) for v in OPENING if v[0] == "f") == C // 2 - 2
    aligned = covered and C == 2 * R and R % 2 == 0 and STEPS == 2 and NV == NC and (NV // R) % (16 * CHUNKS) == 0 and (NV // R) % 128 == 0 and (NC // C) % 128 == 0
    body = (lambda *args: fused_shards(R, C, *args)) if aligned else shards
    return jax.shard_map(
        body,
        mesh=mesh,
        in_specs=(
            P("row", "col"),
            P("row"),
            P("col"),
            P("row", "col"),
            P("col", "row"),
            P("row", "col"),
        ),
        out_specs=(P("row", "col"), P()),
        check_vma=False,
    )
```
